32 devices in a mesh: vol: 8 (over z, y), pix: 4 (over x, core).
Axes of the slice: x: 2, y: 2, z: 4, core: 2. Of those that a mesh axis runs over, the one named last changes fastest.
Arguments:
- kernel: bfloat16 [524288, 128], P(('vol', 'pix')), may hold values from 0 to 0.25
- pressure: bfloat16 [524288], P(('vol', 'pix')), may hold values from 0.049804688 to 2
- velocity: bfloat16 [524288], P(('vol', 'pix')), may hold values from -4 to 4
- entry_slot: int32 [32, 16384], P(('vol', 'pix')), may hold values from 0 to 1023, never falling along the last dimension, each value on 1 to 32 neighbouring positions
- slot_tile: int32 [32, 1024], P(('vol', 'pix')), may hold values from 0 to 8191, as said below
- tile_owner: int32 [8192], replicated, may hold values from 0 to 3, as said below
Outputs:
- owned_tiles: float32 [16384, 256], P(('vol', 'pix'))
- shell_map: float32 [8192, 256], P('vol')
The draws below stay inside these ranges and needn't reach their ends.
Inputs may be any that keep to these rules, and one draw needn't show every extreme that they name: `entry_slot`: for each device the slot numbers never fall along its 16384 crossings; every slot has at least one crossing and at most 32. `tile_owner`: within every block of 1024 consecutive tiles each pix index owns 256 // 2 to 512 tiles, and one owner of each block owns exactly 512. `slot_tile`: the 1024 tiles of one device are distinct; at most 64 of them belong to any one owning device (vol index t // 1024, pix index tile_owner[t]), and one owning device gets exactly 64 from every device.
All inputs are finite; a program needn't handle non-finite values.
Results may differ from the reference program's by a relative error of at most 0.0003.
Values sent between devices are 32-bit elements; how exact they have to be, the bound alone decides.
No kernel may reach another device: no remote copies, remote signals or barrier semaphores. Data moves between devices by JAX's collectives and lax.ppermute only.
A program may use at most 64 MiB of HBM per device.

```python
import math
import jax
import jax.numpy as jnp
import numpy as np
from jax import lax

PIX_TILE = 128
CHANNELS = 2
ENTRIES = 16384
SLOTS = 1024
TILE_DEV = 256
TILE_V = 1024
TILES = 8192
OWN_MAX = 512
CAP = 64
N_VOL = 8
N_PIX = 4
DEVICES = 32


def ownership(key):
    groups = TILE_V // TILE_DEV
    vol_count = TILES // TILE_V
    least_owned = TILE_DEV // 2
    most_owned = 2 * TILE_DEV
    remainder = TILE_V - most_owned - (groups - 1) * least_owned
    labels = jnp.arange(groups, dtype=jnp.int32)

    def one_block(block_key):
        busiest_key, pool_key, mix_key = jax.random.split(block_key, 3)
        busiest = jax.random.randint(busiest_key, (), 0, groups, dtype=jnp.int32)
        baseline = jnp.repeat(labels, least_owned)
        extra_top = jnp.full((most_owned - least_owned,), 1, jnp.int32) * busiest
        token_pool = jax.random.permutation(pool_key, jnp.repeat(labels, most_owned - least_owned))
        ordering = jnp.argsort((token_pool == busiest).astype(jnp.int32), stable=True)
        chosen = token_pool[ordering][:remainder]
        block_owner = jnp.concatenate([baseline, extra_top, chosen]).astype(jnp.int32)
        return (jax.random.permutation(mix_key, block_owner), busiest)
    owners, busiest_overall = jax.vmap(one_block)(jax.random.split(key, vol_count))
    heavy_vol = jax.random.randint(jax.random.fold_in(key, 7), (), 0, vol_count, dtype=jnp.int32)
    heavy_device = heavy_vol * groups + busiest_overall[heavy_vol]
    return (owners.astype(jnp.int32), heavy_device.astype(jnp.int32))


def draw_tile_owner(key, part):
    owners, heavy_device = ownership(jax.random.fold_in(key, 101))
    return owners.reshape(TILES)


def draw_slot_tile(key, part):
    owners, heavy_device = ownership(jax.random.fold_in(key, 101))
    groups = TILE_V // TILE_DEV
    vol_count = TILES // TILE_V
    device_count = vol_count * groups
    flat_owner = owners.reshape(TILES)
    holder = jnp.arange(TILES, dtype=jnp.int32) // TILE_V * groups + flat_owner
    held_count = jax.ops.segment_sum(jnp.ones((TILES,), jnp.int32), holder, num_segments=device_count)
    first_row = (jnp.cumsum(held_count, dtype=jnp.int32) - held_count).astype(jnp.int32)
    labels = jnp.arange(device_count, dtype=jnp.int32)

    def one_device(device_key):
        pool_key, ranking_random_key, mix_key = jax.random.split(device_key, 3)
        token_pool = jax.random.permutation(pool_key, jnp.repeat(labels, CAP))
        ordering = jnp.argsort((token_pool == heavy_device).astype(jnp.int32), stable=True)
        chosen = token_pool[ordering][:SLOTS - CAP]
        wanted = jax.ops.segment_sum(jnp.ones((SLOTS - CAP,), jnp.int32), chosen, num_segments=device_count)
        wanted = wanted + CAP * (labels == heavy_device).astype(jnp.int32)
        shuffle = jax.random.permutation(ranking_random_key, TILES).astype(jnp.int32)
        grouped = jnp.argsort(holder * TILES + shuffle, stable=True).astype(jnp.int32)
        position = jnp.arange(TILES, dtype=jnp.int32) - first_row[holder[grouped]]
        selected = position < wanted[holder[grouped]]
        positions = jnp.nonzero(selected, size=SLOTS)[0]
        tile_ids = grouped[positions].astype(jnp.int32)
        return jax.random.permutation(mix_key, tile_ids)
    device_keys = jax.random.split(jax.random.fold_in(key, 202), device_count)
    return jax.vmap(one_device)(device_keys).astype(jnp.int32)


def levels(rng, dims, cuts, low, high):
    def one(axis_at, blocks):
        heights = jax.random.uniform(jax.random.fold_in(jax.random.fold_in(rng, 6), axis_at), (blocks,), jnp.float32, low / len(cuts), high / len(cuts))
        return jnp.repeat(jnp.exp(heights), dims[axis_at] // blocks).reshape((-1,) + (1,) * (len(dims) - axis_at - 1))

    factor_of = one(*cuts[0])
    for cut in cuts[1:]:
        factor_of = factor_of * one(*cut)
    return factor_of


def profile(number_of, total, limit, skew):
    loads = [(1 << 20) // math.isqrt(rank ** skew) + 1 for rank in range(2, number_of + 1)]
    spare, counts = total - limit - (number_of - 1), [1] * (number_of - 1)
    while spare > 0:
        candidates = [i for i in range(number_of - 1) if counts[i] < limit]
        pool, left = sum([loads[i] for i in candidates]), spare
        for i in candidates:
            more = min(limit - counts[i], max(1, left * loads[i] // pool), spare)
            counts[i] = counts[i] + more
            spare = spare - more
    return np.array([limit] + counts)


def ragged(stream_key, number_of, total, limit, slope):
    if number_of == 2:
        one = jax.random.randint(stream_key, (), max(1, total - limit), min(limit, total - 1) + 1)
        return jnp.stack([one, total - one])
    tallies = jnp.asarray(profile(number_of, total, limit, slope), jnp.int32)
    twos = (number_of - 1) // 2
    donor, receiver = tallies[1:1 + 2 * twos:2], tallies[2:2 + 2 * twos:2]
    margin = jnp.minimum(donor - 1, limit - receiver)
    passed = jax.random.randint(jax.random.fold_in(stream_key, 1), (twos,), 0, 1 << 20) % (margin + 1)
    tallies = tallies.at[1:1 + 2 * twos:2].set(donor - passed).at[2:2 + 2 * twos:2].set(receiver + passed)
    return tallies[jax.random.permutation(jax.random.fold_in(stream_key, 2), number_of)]


def normal_values(rng, shape, spread, reach, shards=(), kind=jnp.bfloat16):
    loudness = levels(rng, shape, shards, -0.22, 0.18) if shards else 1.0
    values = jax.random.normal(rng, shape, jnp.float32) * spread * loudness
    return jnp.minimum(jnp.maximum(values, -reach), reach).astype(kind)


def setup_inputs(seed: int = 0) -> dict:
    splits = jax.random.split(jax.random.key(seed), 7)
    return {
        "kernel": jnp.clip(0.25 * jax.random.uniform(splits[0], (DEVICES * ENTRIES, PIX_TILE), jnp.float32) ** levels(splits[0], (DEVICES * ENTRIES, PIX_TILE), ((0, 32),), -0.2, 0.2), 0.0, 0.25).astype(jnp.bfloat16),
        "pressure": jnp.clip(jnp.exp(math.log(2.0) - 3.6927934 * jax.random.uniform(splits[1], (DEVICES * ENTRIES,), jnp.float32) ** levels(splits[1], (DEVICES * ENTRIES,), ((0, 32),), -0.2, 0.2)), 0.049804688, 2.0).astype(jnp.bfloat16),
        "velocity": normal_values(splits[2], (DEVICES * ENTRIES,), 1.0, 4.0, ((0, 32),)),
        "entry_slot": jax.vmap(lambda own: jnp.searchsorted(jnp.cumsum(ragged(own, SLOTS, ENTRIES, 2 * ENTRIES // SLOTS, 1)), jnp.arange(ENTRIES), side="right"))(jax.random.split(splits[3], DEVICES)).reshape((DEVICES, ENTRIES)).astype(jnp.int32),
        "slot_tile": draw_slot_tile(jax.random.fold_in(splits[6], 71), 0),
        "tile_owner": draw_tile_owner(jax.random.fold_in(splits[6], 71), 0),
    }


def reference(kernel, pressure, velocity, entry_slot, slot_tile, tile_owner):
    kernel_weights = kernel.reshape(DEVICES, ENTRIES, PIX_TILE)
    amplitude = jnp.stack([pressure, velocity], axis=-1).reshape(DEVICES, ENTRIES, CHANNELS)

    def accumulate(running, inputs):
        device_kernel, device_amplitude, device_slot, device_tile = inputs
        pixel_products = device_amplitude.astype(jnp.float32)[:, :, None] * device_kernel.astype(jnp.float32)[:, None, :]
        partial_value = jax.ops.segment_sum(pixel_products.reshape(ENTRIES, CHANNELS * PIX_TILE), device_slot, num_segments=SLOTS)
        return running.at[device_tile].add(partial_value), None

    start_value = jnp.zeros((TILES, CHANNELS * PIX_TILE), jnp.float32)
    shell_map, unused = lax.scan(accumulate, start_value, (kernel_weights, amplitude, entry_slot, slot_tile))
    owners = tile_owner.reshape(N_VOL, TILE_V)
    matches = owners[:, None, :] == jnp.arange(N_PIX, dtype=jnp.int32)[None, :, None]
    owner_ranking = jnp.cumsum(matches.astype(jnp.int32), axis=2, dtype=jnp.int32) - 1
    owner_rank = jnp.sum(jnp.where(matches, owner_ranking, 0), axis=1, dtype=jnp.int32)
    vol_ids = jnp.arange(N_VOL, dtype=jnp.int32)[:, None]
    destination = ((vol_ids * N_PIX + owners) * OWN_MAX + owner_rank).astype(jnp.int32)
    owned_tiles = jnp.zeros((DEVICES * OWN_MAX, CHANNELS * PIX_TILE), jnp.float32)
    owned_tiles = owned_tiles.at[destination.reshape(TILES)].set(shell_map)
    return owned_tiles, shell_map
```

```python
import functools

import jax
import jax.numpy as jnp
from jax import lax
from jax.experimental import pallas as pl
from jax.experimental.pallas import tpu as pltpu
from jax.sharding import PartitionSpec as P

LANES = 128
HEAD = 8
GROUP = 256
WINDOW = 40


def whole(shape):
    return pl.BlockSpec(shape, lambda *_: (0,) * len(shape))


SMEM = pl.BlockSpec(memory_space=pltpu.SMEM)
VMEM = pl.BlockSpec(memory_space=pltpu.VMEM)


def iota(shape, axis):
    return lax.broadcasted_iota(jnp.int32, shape, axis)


def nt_dot(a, b):
    return lax.dot_general(a, b, (((1,), (1,)), ((), ())), preferred_element_type=jnp.float32)


def dot(a, b):
    return jnp.dot(a, b, preferred_element_type=jnp.float32)


def ones_where(mask):
    return jnp.where(mask, 1.0, 0.0).astype(jnp.bfloat16)


def running_counts(marks, rows):
    total = marks.shape[0]
    upper = ones_where(iota((LANES, LANES), 0) <= iota((LANES, LANES), 1))
    row, column = iota((total, total), 0), iota((total, total), 1)
    earlier = ones_where((column < row) & (row // rows == column // rows))
    before = dot(earlier, marks).astype(jnp.bfloat16)
    return dot(marks, upper) + dot(before, jnp.ones((LANES, LANES), jnp.bfloat16))


def plan_kernel(vols, block, cap, me_ref, tile_ref, place_ref, head_ref):
    me = me_ref[0]
    tiles = tile_ref[...]
    rows = tiles.shape[0]
    vol = tiles // block
    local = tiles - vol * block + 1
    marks = jnp.concatenate([jnp.where(vol == i, 1.0, 0.0) for i in range(vols)], axis=0)
    counts = running_counts(marks.astype(jnp.bfloat16), rows) * marks
    place = jnp.zeros((rows, LANES), jnp.float32)
    for i in range(vols):
        place = place + counts[i * rows : (i + 1) * rows]
    place = place.astype(jnp.int32) - 1
    fits = place < cap
    bucket = vol ^ me
    place_ref[...] = jnp.where(fits, bucket * (cap + HEAD) + place, vols * (cap + HEAD))
    spilled = jnp.sum(jnp.where(fits, 0.0, 1.0), axis=(0, 1), keepdims=True)
    width = head_ref.shape[2]
    high = (local // 64).astype(jnp.float32)
    low = (local % 64).astype(jnp.float32)
    ids = jnp.zeros((2 * vols, width), jnp.float32)
    which = iota((vols, LANES), 0)
    for r in range(rows):
        here = (bucket[r : r + 1] == which) & fits[r : r + 1]
        parts = jnp.concatenate(
            [jnp.where(here, high[r : r + 1], 0.0), jnp.where(here, low[r : r + 1], 0.0)], axis=0
        )
        slots = ones_where(iota((width, LANES), 0) == place[r : r + 1])
        ids = ids + nt_dot(parts.astype(jnp.bfloat16), slots)
    ids = ids[:vols] * 64.0 + ids[vols:] - 1.0
    line = iota((HEAD, width), 0)
    for k in range(vols):
        head_ref[k] = jnp.where(
            line == 0, ids[k : k + 1], jnp.where(line == 1, jnp.broadcast_to(spilled, (HEAD, width)), 0.0)
        )


def plan(me, tiles, vols, block, cap, width):
    rows = tiles.shape[0]
    return pl.pallas_call(
        functools.partial(plan_kernel, vols, block, cap),
        in_specs=[SMEM, VMEM],
        out_specs=[VMEM, VMEM],
        out_shape=[
            jax.ShapeDtypeStruct((rows, LANES), jnp.int32),
            jax.ShapeDtypeStruct((vols, HEAD, width), jnp.float32),
        ],
        name="plan",
    )(me, tiles)


def project_kernel(
    steps, vols, cap, base_ref, turns_ref, place_ref, kernel_ref, thermal_ref, kinetic_ref, slot_ref, head_ref, *rest
):
    outs, (partial_ref, stage_ref, thermal_s, kinetic_s) = rest[:vols], rest[vols:]
    step = pl.program_id(0)
    pixels = kernel_ref.shape[1]
    groups = kernel_ref.shape[0] // GROUP
    lines = GROUP // LANES
    slots = place_ref.shape[0]

    @pl.when(step == 0)
    def _():
        partial_ref[...] = jnp.zeros_like(partial_ref)
        stage_ref[...] = jnp.zeros_like(stage_ref)

    thermal_s[...] = thermal_ref[...].astype(jnp.float32)
    kinetic_s[...] = kinetic_ref[...].astype(jnp.float32)
    line = iota((WINDOW, LANES), 0)

    def add(group, start, base):
        top, low = [], []
        for r in range(lines):
            row = pl.ds(group * lines + r, 1)
            match = line == slot_ref[row, :] - base
            top.append(jnp.where(match, thermal_s[row, :], 0.0))
            low.append(jnp.where(match, kinetic_s[row, :], 0.0))
        weights = jnp.concatenate(
            [jnp.concatenate(top, axis=1), jnp.concatenate(low, axis=1)], axis=0
        ).astype(jnp.bfloat16)
        sums = dot(weights, kernel_ref[pl.ds(start, GROUP), :])
        window = pl.ds(pl.multiple_of(base, 8), WINDOW)
        partial_ref[window, :pixels] += sums[:WINDOW]
        partial_ref[window, pixels:] += sums[WINDOW:]

    most = turns_ref[step * groups]
    for g in range(groups):
        add(g, g * GROUP, base_ref[step * groups + g])
        if g:
            most = jnp.maximum(most, turns_ref[step * groups + g])

    @pl.when(most > 1)
    def _():
        def more(g, carry):
            def turn(w, inner):
                add(g, pl.multiple_of(g * GROUP, GROUP), base_ref[step * groups + g] + w * WINDOW)
                return inner

            return lax.fori_loop(1, turns_ref[step * groups + g], turn, carry)

        lax.fori_loop(0, groups, more, 0)

    @pl.when(step == steps - 1)
    def _():
        unroll = 16

        def move(i, carry):
            for u in range(unroll):
                s = i * unroll + u
                stage_ref[pl.ds(place_ref[s], 1), :] = partial_ref[pl.ds(s, 1), :]
            return carry

        lax.fori_loop(0, slots // unroll, move, 0)
        for k in range(vols):
            outs[k][:cap, :] = stage_ref[k * (cap + HEAD) : k * (cap + HEAD) + cap, :]
            outs[k][cap:, :] = head_ref[k]


def project(kernel, thermal, kinetic, slot, base, turns, place, head, vols, cap):
    entries, pixels = kernel.shape
    slots = place.shape[0]
    width = 2 * pixels
    steps = 4
    rows = entries // LANES // steps
    return pl.pallas_call(
        functools.partial(project_kernel, steps, vols, cap),
        grid_spec=pltpu.PrefetchScalarGridSpec(
            num_scalar_prefetch=3,
            grid=(steps,),
            in_specs=[
                pl.BlockSpec((entries // steps, pixels), lambda i, *_: (i, 0)),
                pl.BlockSpec((rows, LANES), lambda i, *_: (i, 0)),
                pl.BlockSpec((rows, LANES), lambda i, *_: (i, 0)),
                pl.BlockSpec((rows, LANES), lambda i, *_: (i, 0)),
                whole(head.shape),
            ],
            out_specs=[whole((cap + HEAD, width))] * vols,
            scratch_shapes=[
                pltpu.VMEM((slots + WINDOW, width), jnp.float32),
                pltpu.VMEM((vols * (cap + HEAD) + HEAD, width), jnp.float32),
                pltpu.VMEM((rows, LANES), jnp.float32),
                pltpu.VMEM((rows, LANES), jnp.float32),
            ],
        ),
        out_shape=[jax.ShapeDtypeStruct((cap + HEAD, width), jnp.float32)] * vols,
        name="project",
    )(base, turns, place, kernel, thermal, kinetic, slot, head)


def split(x):
    high = x.astype(jnp.bfloat16)
    return high, (x - high.astype(jnp.float32)).astype(jnp.bfloat16)


def gather_kernel(count, cap, first, last, block, *refs):
    core_ref, refs = (refs[0], refs[1:]) if last else (None, refs)
    buckets, refs = refs[:count], refs[count:]
    held_ref, refs = (None, refs) if first else (refs[0], refs[1:])
    width = buckets[0].shape[1]
    pixels = width // 2
    high_s, low_s = refs[-2:]
    flag = jnp.zeros((HEAD, width), jnp.float32)
    ids = []
    for b, bucket in enumerate(buckets):
        high, low = split(bucket[:cap, :])
        high_s[b], low_s[b] = high, low
        head = bucket[cap:, :]
        flag = flag + head[1:2]
        ids.append(head[0:1, :cap].astype(jnp.int32))
    chunk = 256
    if held_ref is not None:
        flag = flag + held_ref[block:, :]
    pieces = [(t, min(chunk, block - t)) for t in range(0, block, chunk)]
    for t, rows in pieces + [(block, HEAD)]:
        if t == block:
            total = flag
        else:
            total = jnp.zeros((rows, width), jnp.float32) if held_ref is None else held_ref[t : t + rows, :]
            for b in range(count):
                ids_b = ids[b]
                hit = ones_where(iota((rows, cap), 0) + t == ids_b)
                total = total + dot(hit, high_s[b])
                total = total + dot(hit, low_s[b])
        if last:
            core = core_ref[0]
            keep_ref, send_ref = refs[0], refs[1]
            one, two = total[:, :pixels], total[:, pixels:]
            keep_ref[t : t + rows, :] = jnp.where(core == 0, one, two)
            send_ref[t : t + rows, :] = jnp.where(core == 0, two, one)
        else:
            refs[0][t : t + rows, :] = total


def collect(buckets, held, core, cap, block):
    width = buckets[0].shape[1]
    last = core is not None
    rows = block + HEAD
    args = ([core] if last else []) + list(buckets) + ([] if held is None else [held])
    outs = [jax.ShapeDtypeStruct((rows, width // 2), jnp.float32)] * 2 if last else jax.ShapeDtypeStruct((rows, width), jnp.float32)
    return pl.pallas_call(
        functools.partial(gather_kernel, len(buckets), cap, held is None, last, block),
        in_specs=([SMEM] if last else []) + [VMEM] * (len(args) - last),
        out_specs=[VMEM] * 2 if last else VMEM,
        out_shape=outs,
        scratch_shapes=[pltpu.VMEM((len(buckets), cap, width), jnp.bfloat16)] * 2,
        name="collect_last" if last else "collect",
    )(*args)


def owner_kernel(most, pix_ref, owner_ref, row_ref):
    owners = owner_ref[...]
    rows = owners.shape[0]
    mine = owners == pix_ref[0]
    marks = jnp.where(mine, 1.0, 0.0)
    rank = running_counts(marks.astype(jnp.bfloat16), rows).astype(jnp.int32) - 1
    index = iota((rows, LANES), 0) * LANES + iota((rows, LANES), 1) + 1
    found = jnp.zeros((HEAD, most), jnp.float32)
    part = iota((HEAD, LANES), 0)
    for r in range(rows):
        here = mine[r : r + 1]
        high = jnp.where(here, (index[r : r + 1] // 64).astype(jnp.float32), 0.0)
        low = jnp.where(here, (index[r : r + 1] % 64).astype(jnp.float32), 0.0)
        parts = jnp.where(part == 0, high, jnp.where(part == 1, low, 0.0))
        spots = ones_where(iota((most, LANES), 0) == rank[r : r + 1])
        found = found + nt_dot(parts.astype(jnp.bfloat16), spots)
    tile = (found[0:1] * 64.0 + found[1:2]).astype(jnp.int32) - 1
    tile = jnp.where(tile < 0, rows * LANES, tile)
    row_ref[...] = jnp.broadcast_to(tile, (HEAD, most))


def owned_rows(pix, owners, most):
    return pl.pallas_call(
        functools.partial(owner_kernel, most),
        in_specs=[SMEM, VMEM],
        out_specs=VMEM,
        out_shape=jax.ShapeDtypeStruct((HEAD, most), jnp.int32),
        name="owned_rows",
    )(pix, owners)


def finish_kernel(core_ref, row_ref, mine_ref, other_ref, owned_ref, map_ref, full_ref):
    block, width = map_ref.shape
    pixels = width // 2
    core = core_ref[0]
    mine, other = mine_ref[:block, :], other_ref[:block, :]
    full_ref[:block, :pixels] = jnp.where(core == 0, mine, other)
    full_ref[:block, pixels:] = jnp.where(core == 0, other, mine)
    full_ref[block:, :] = jnp.zeros((HEAD, width), jnp.float32)
    map_ref[...] = full_ref[:block, :]
    unroll = 16

    def move(i, carry):
        for u in range(unroll):
            r = i * unroll + u
            owned_ref[pl.ds(r, 1), :] = full_ref[pl.ds(row_ref[r], 1), :]
        return carry

    lax.fori_loop(0, owned_ref.shape[0] // unroll, move, 0)


def finish(core, rows, mine, other):
    block, pixels = mine.shape[0] - HEAD, mine.shape[1]
    return pl.pallas_call(
        finish_kernel,
        in_specs=[SMEM, SMEM, VMEM, VMEM],
        out_specs=[VMEM, VMEM],
        out_shape=[
            jax.ShapeDtypeStruct((rows.shape[0], 2 * pixels), jnp.float32),
            jax.ShapeDtypeStruct((block, 2 * pixels), jnp.float32),
        ],
        scratch_shapes=[pltpu.VMEM((block + HEAD, 2 * pixels), jnp.float32)],
        name="finish",
    )(core, rows, mine, other)


def shards(kernel, pressure, velocity, entry_slot, slot_tile, tile_owner):
    vols = lax.axis_size("vol")
    pixs = lax.axis_size("pix")
    vol = lax.axis_index("vol")
    pix = lax.axis_index("pix")
    entries, pixels = kernel.shape
    slots = slot_tile.shape[1]
    block = tile_owner.shape[0] // vols
    most_owned = 2 * block // pixs
    most_rows = 2 * slots // vols
    width = 2 * pixels
    scalar = lambda x: jnp.asarray(x, jnp.int32).reshape(1)
    tiles = slot_tile.reshape(slots // LANES, LANES)
    slot = entry_slot.reshape(entries // LANES, LANES)
    thermal = pressure.reshape(entries // LANES, LANES)
    kinetic = velocity.reshape(entries // LANES, LANES)
    ends = entry_slot.reshape(entries // GROUP, GROUP)
    base = ends[:, 0] // 8 * 8
    turns = (ends[:, GROUP - 1] - base) // WINDOW + 1
    core = scalar(pix % 2)
    owners = lax.dynamic_slice_in_dim(tile_owner, vol * block, block)
    rows = owned_rows(scalar(pix), owners.reshape(block // LANES, LANES), most_owned)[0]

    def exchange(cap):
        place, head = plan(scalar(vol), tiles, vols, block, cap, width)
        buckets = project(
            kernel, thermal, kinetic, slot, base, turns, place.reshape(slots), head, vols, cap
        )
        arrived = {
            k: lax.ppermute(buckets[k], "vol", [(d, d ^ k) for d in range(vols)])
            for k in reversed(range(1, vols))
        }
        arrived[0] = buckets[0]
        order = list(range(vols))
        half = vols // 2
        held = collect([arrived[k] for k in order[:half]], None, None, cap, block)
        keep, send = collect([arrived[k] for k in order[half:]], held, core, cap, block)
        pairs = [(p, p ^ 1) for p in range(pixs)]
        mine = keep + lax.ppermute(send, "pix", pairs)
        step = 2
        while step < pixs:
            mine = mine + lax.ppermute(mine, "pix", [(p, p ^ step) for p in range(pixs)])
            step *= 2
        other = lax.ppermute(mine, "pix", pairs)
        return mine, other

    mine, other = exchange(most_rows * 23 // 32 // 8 * 8)
    spilled = mine[block, 0] > 0
    owned, shell = lax.cond(
        spilled,
        lambda: finish(core, rows, *exchange(most_rows)),
        lambda: finish(core, rows, mine, other),
    )
    return owned, shell


def solution(mesh):
    in_specs = (
        P(("vol", "pix"), None),
        P(("vol", "pix")),
        P(("vol", "pix")),
        P(("vol", "pix"), None),
        P(("vol", "pix"), None),
        P(),
    )
    out_specs = (P(("vol", "pix"), None), P("vol", None))
    return jax.shard_map(shards, mesh=mesh, in_specs=in_specs, out_specs=out_specs, check_vma=False)
```

```python
import functools

import jax
import jax.numpy as jnp
from jax import lax
from jax.experimental import pallas as pl
from jax.experimental.pallas import tpu as pltpu
from jax.sharding import PartitionSpec as P


LANES = 128
HEAD = 8
ROOM = pltpu.CompilerParams(vmem_limit_bytes=16 << 20)
GROUP = 256
WINDOW = 40


SMEM = pl.BlockSpec(memory_space=pltpu.SMEM)
VMEM = pl.BlockSpec(memory_space=pltpu.VMEM)
ANY = pl.BlockSpec(memory_space=pl.ANY)
HBM = pl.BlockSpec(memory_space=pltpu.HBM)


def iota(shape, axis):
    return lax.broadcasted_iota(jnp.int32, shape, axis)


def nt_dot(a, b):
    return lax.dot_general(a, b, (((1,), (1,)), ((), ())), preferred_element_type=jnp.float32)


def dot(a, b):
    return jnp.dot(a, b, preferred_element_type=jnp.float32)


def ones_where(mask):
    return jnp.where(mask, 1.0, 0.0).astype(jnp.bfloat16)


def running_counts(marks, rows):
    total = marks.shape[0]
    upper = ones_where(iota((LANES, LANES), 0) <= iota((LANES, LANES), 1))
    row, column = iota((total, total), 0), iota((total, total), 1)
    earlier = ones_where((column < row) & (row // rows == column // rows))
    before = dot(earlier, marks).astype(jnp.bfloat16)
    return dot(marks, upper) + dot(before, jnp.ones((LANES, LANES), jnp.bfloat16))


def plan_kernel(vols, block, cap, me_ref, tile_ref, slot_ref, place_ref, ends_ref, head_ref):
    lane = iota((HEAD, LANES), 1)
    line = iota((HEAD, LANES), 0)
    slots = slot_ref[...]
    ends = ones_where(((line == 0) & (lane == 0)) | ((line == 1) & (lane == LANES - 1)))
    high = nt_dot(ends, (slots // 64).astype(jnp.float32).astype(jnp.bfloat16))
    low = nt_dot(ends, (slots % 64).astype(jnp.float32).astype(jnp.bfloat16))
    ends_ref[...] = (high * 64.0 + low).astype(jnp.int32)

    me = me_ref[0]
    tiles = tile_ref[...]
    rows = tiles.shape[0]
    vol = tiles // block
    local = tiles - vol * block + 1
    marks = jnp.concatenate([jnp.where(vol == i, 1.0, 0.0) for i in range(vols)], axis=0)
    counts = running_counts(marks.astype(jnp.bfloat16), rows) * marks
    place = jnp.zeros((rows, LANES), jnp.float32)
    for i in range(vols):
        place = place + counts[i * rows : (i + 1) * rows]
    place = place.astype(jnp.int32) - 1
    fits = place < cap
    bucket = vol ^ me
    place_ref[...] = jnp.where(fits, bucket * (cap + HEAD) + place, vols * (cap + HEAD))
    spilled = jnp.sum(jnp.where(fits, 0.0, 1.0), axis=(0, 1), keepdims=True)
    lists = -(-cap // LANES)
    width = lists * LANES
    high = (local // 64).astype(jnp.float32)
    low = (local % 64).astype(jnp.float32)
    ids = jnp.zeros((2 * vols, width), jnp.float32)
    which = iota((vols, LANES), 0)
    for r in range(rows):
        here = (bucket[r : r + 1] == which) & fits[r : r + 1]
        parts = jnp.concatenate(
            [jnp.where(here, high[r : r + 1], 0.0), jnp.where(here, low[r : r + 1], 0.0)], axis=0
        )
        spots = ones_where(iota((width, LANES), 0) == place[r : r + 1])
        ids = ids + nt_dot(parts.astype(jnp.bfloat16), spots)
    ids = ids[:vols] * 64.0 + ids[vols:] - 1.0
    for k in range(vols):
        head = jnp.where(line == lists, jnp.broadcast_to(spilled, (HEAD, LANES)), 0.0)
        for i in range(lists):
            head = jnp.where(line == i, ids[k : k + 1, i * LANES : (i + 1) * LANES], head)
        head_ref[k * HEAD : (k + 1) * HEAD, :] = head


def plan(me, tiles, slot, vols, block, cap):
    rows = tiles.shape[0]
    return pl.pallas_call(
        functools.partial(plan_kernel, vols, block, cap),
        in_specs=[SMEM, VMEM, VMEM],
        out_specs=[VMEM, VMEM, VMEM],
        out_shape=[
            jax.ShapeDtypeStruct((rows, LANES), jnp.int32),
            jax.ShapeDtypeStruct((HEAD, slot.shape[0]), jnp.int32),
            jax.ShapeDtypeStruct((vols * HEAD, LANES), jnp.float32),
        ],
        compiler_params=ROOM,
        name="plan",
    )(me, tiles, slot)


def project_kernel(steps, vols, cap, ends_ref, place_ref, kernel_hbm, factor_ref, slot_ref, head_ref, *rest):
    outs, (kernel_ref, partial_ref, stage_ref, factor_s, in_sem) = rest[:vols], rest[vols:]
    entries, _ = kernel_ref.shape
    part = entries // steps
    groups = part // GROUP
    lines = GROUP // LANES
    slots = place_ref.shape[0]
    total = entries // LANES
    size = cap + HEAD

    def load(step):
        piece = pl.ds(pl.multiple_of(step * part, part), part)
        return pltpu.make_async_copy(kernel_hbm.at[piece], kernel_ref.at[piece], in_sem.at[step])

    for step in range(steps):
        load(step).start()
    partial_ref[...] = jnp.zeros_like(partial_ref)
    stage_ref[...] = jnp.zeros_like(stage_ref)
    factor_s[...] = factor_ref[...].astype(jnp.float32)
    line = iota((WINDOW, LANES), 0)

    def first(group):
        return ends_ref[group * lines] & -8

    def reach(group):
        return ends_ref[total + group * lines + lines - 1] - first(group)

    def add(group, base):
        row = []
        for r in range(lines):
            at = pl.ds(group * lines + r, 1)
            row.append(jnp.where(line == slot_ref[at, :] - base, factor_s[at, :], 0.0))
        weights = jnp.concatenate(row, axis=1).astype(jnp.bfloat16)
        sums = dot(weights, kernel_ref[pl.ds(pl.multiple_of(group * GROUP, GROUP), GROUP), :])
        partial_ref[pl.ds(pl.multiple_of(base, 8), WINDOW), :] += sums

    def turn(step, most):
        load(step).wait()
        for g in range(groups):
            group = step * groups + g
            add(group, first(group))
            most = jnp.maximum(most, reach(group))
        return most

    most = lax.fori_loop(0, steps, turn, 0)

    @pl.when(most >= WINDOW)
    def _():
        def more(group, carry):
            def again(w, inner):
                add(group, first(group) + w * WINDOW)
                return inner

            return lax.fori_loop(1, reach(group) // WINDOW + 1, again, carry)

        lax.fori_loop(0, steps * groups, more, 0)

    unroll = 16

    def move(i, carry):
        for u in range(unroll):
            s = i * unroll + u
            stage_ref[pl.ds(place_ref[s], 1), :] = partial_ref[pl.ds(s, 1), :]
        return carry

    lax.fori_loop(0, slots // unroll, move, 0)
    for k in range(vols):
        outs[k][:cap, :] = stage_ref[k * size : k * size + cap, :]
        outs[k][cap:, :] = head_ref[k * HEAD : (k + 1) * HEAD, :]


def project(kernel, factor, slot, ends, place, head, vols, cap):
    entries, pixels = kernel.shape
    slots = place.shape[0]
    steps = 4
    size = cap + HEAD
    return pl.pallas_call(
        functools.partial(project_kernel, steps, vols, cap),
        in_specs=[SMEM, SMEM, HBM, VMEM, VMEM, VMEM],
        out_specs=[VMEM] * vols,
        out_shape=[jax.ShapeDtypeStruct((size, pixels), jnp.float32)] * vols,
        scratch_shapes=[
            pltpu.VMEM((entries, pixels), kernel.dtype),
            pltpu.VMEM((slots + WINDOW, pixels), jnp.float32),
            pltpu.VMEM((vols * size + HEAD, pixels), jnp.float32),
            pltpu.VMEM(factor.shape, jnp.float32),
            pltpu.SemaphoreType.DMA((steps,)),
        ],
        compiler_params=ROOM,
        name="project",
    )(ends, place, kernel, factor, slot, head)


def split(x):
    high = x.astype(jnp.bfloat16)
    return high, (x - high.astype(jnp.float32)).astype(jnp.bfloat16)


def collect_kernel(count, cap, first, last, block, *refs):
    core_ref, refs = (refs[0], refs[1:]) if last else (None, refs)
    buckets, refs = refs[:count], refs[count:]
    held_ref, refs = (None, refs) if first else (refs[0], refs[1:])
    pixels = buckets[0].shape[1]
    lists = -(-cap // LANES)
    outs, rows_s = refs[:-1], refs[-1]
    flag = jnp.zeros((HEAD, pixels), jnp.float32)
    ids = []
    for b, bucket in enumerate(buckets):
        rows_s[b] = jnp.concatenate(split(bucket[:cap, :]), axis=1)
        head = bucket[cap:, :]
        flag = flag + head[lists : lists + 1]
        names = [head[i : i + 1] for i in range(lists)]
        ids.append(jnp.concatenate(names, axis=1)[:, :cap].astype(jnp.int32))
    if held_ref is not None:
        flag = flag + held_ref[block:, :]

    def total(t, rows):
        sums = jnp.zeros((rows, 2 * pixels), jnp.float32)
        for b in range(count):
            sums = sums + dot(ones_where(iota((rows, cap), 0) + t == ids[b]), rows_s[b])
        sums = sums[:, :pixels] + sums[:, pixels:]
        return sums if held_ref is None else sums + held_ref[t : t + rows, :]

    chunk = 256
    if not last:
        for t in range(0, block, chunk):
            outs[0][t : t + chunk, :] = total(t, chunk)
        outs[0][block:, :] = flag
        return
    keep_ref, send_ref = outs
    lower = core_ref[0] == 0
    half = block // 2
    for t in range(0, half, chunk):
        one, two = total(t, chunk), total(t + half, chunk)
        keep_ref[t : t + chunk, :] = jnp.where(lower, one, two)
        send_ref[t : t + chunk, :] = jnp.where(lower, two, one)
    keep_ref[half:, :] = flag
    send_ref[half:, :] = flag


def collect(buckets, held, core, cap, block):
    pixels = buckets[0].shape[1]
    last = core is not None
    args = ([core] if last else []) + list(buckets) + ([] if held is None else [held])
    rows = block // 2 + HEAD if last else block + HEAD
    out = jax.ShapeDtypeStruct((rows, pixels), jnp.float32)
    return pl.pallas_call(
        functools.partial(collect_kernel, len(buckets), cap, held is None, last, block),
        in_specs=([SMEM] if last else []) + [VMEM] * (len(args) - last),
        out_specs=[VMEM] * 2 if last else VMEM,
        out_shape=[out] * 2 if last else out,
        scratch_shapes=[pltpu.VMEM((len(buckets), cap, 2 * pixels), jnp.bfloat16)],
        compiler_params=ROOM,
        name="collect_last" if last else "collect",
    )(*args)


def owner_kernel(most, pix_ref, owner_ref, row_ref):
    owners = owner_ref[...]
    rows = owners.shape[0]
    mine = owners == pix_ref[0]
    marks = jnp.where(mine, 1.0, 0.0)
    rank = running_counts(marks.astype(jnp.bfloat16), rows).astype(jnp.int32) - 1
    index = iota((rows, LANES), 0) * LANES + iota((rows, LANES), 1) + 1
    found = jnp.zeros((HEAD, most), jnp.float32)
    part = iota((HEAD, LANES), 0)
    for r in range(rows):
        here = mine[r : r + 1]
        high = jnp.where(here, (index[r : r + 1] // 64).astype(jnp.float32), 0.0)
        low = jnp.where(here, (index[r : r + 1] % 64).astype(jnp.float32), 0.0)
        parts = jnp.where(part == 0, high, jnp.where(part == 1, low, 0.0))
        spots = ones_where(iota((most, LANES), 0) == rank[r : r + 1])
        found = found + nt_dot(parts.astype(jnp.bfloat16), spots)
    tile = (found[0:1] * 64.0 + found[1:2]).astype(jnp.int32) - 1
    tile = jnp.where(tile < 0, rows * LANES, tile)
    row_ref[...] = jnp.broadcast_to(tile, (HEAD, most))


def owned_rows(pix, owners, most):
    return pl.pallas_call(
        functools.partial(owner_kernel, most),
        in_specs=[SMEM, VMEM],
        out_specs=VMEM,
        out_shape=jax.ShapeDtypeStruct((HEAD, most), jnp.int32),
        compiler_params=ROOM,
        name="owned_rows",
    )(pix, owners)


def finish_kernel(channel, core_ref, row_ref, mine_ref, other_ref, *rest):
    owned_ref, map_ref, full_ref, own_ref = rest[-4:]
    half, pixels = mine_ref.shape[0] - HEAD, mine_ref.shape[1]
    columns = slice(channel * pixels, (channel + 1) * pixels)
    core = core_ref[0]
    for at, part in ((core, mine_ref), (1 - core, other_ref)):
        at = pl.ds(pl.multiple_of(at * half, half), half)
        value = part[:half, :]
        full_ref[at, :] = value
        map_ref[at, columns] = value
    full_ref[2 * half :, :] = jnp.zeros((HEAD, pixels), jnp.float32)
    unroll = 16

    def move(i, carry):
        for u in range(unroll):
            r = i * unroll + u
            own_ref[pl.ds(r, 1), :] = full_ref[pl.ds(row_ref[r], 1), :]
        return carry

    lax.fori_loop(0, own_ref.shape[0] // unroll, move, 0)
    owned_ref[:, columns] = own_ref[...]


def finish(channel, core, rows, mine, other, before):
    block, pixels = 2 * (mine.shape[0] - HEAD), mine.shape[1]
    return pl.pallas_call(
        functools.partial(finish_kernel, channel),
        in_specs=[SMEM, SMEM, VMEM, VMEM] + [VMEM] * len(before),
        out_specs=[VMEM, VMEM],
        out_shape=[
            jax.ShapeDtypeStruct((rows.shape[0], 2 * pixels), jnp.float32),
            jax.ShapeDtypeStruct((block, 2 * pixels), jnp.float32),
        ],
        input_output_aliases={4: 0, 5: 1} if before else {},
        scratch_shapes=[
            pltpu.VMEM((block + HEAD, pixels), jnp.float32),
            pltpu.VMEM((rows.shape[0], pixels), jnp.float32),
        ],
        compiler_params=ROOM,
        name="finish",
    )(core, rows, mine, other, *before)


def shards(kernel, pressure, velocity, entry_slot, slot_tile, tile_owner):
    vols = lax.axis_size("vol")
    pixs = lax.axis_size("pix")
    vol = lax.axis_index("vol")
    pix = lax.axis_index("pix")
    entries, _ = kernel.shape
    slots = slot_tile.shape[1]
    block = tile_owner.shape[0] // vols
    most_owned = 2 * block // pixs
    most_rows = 2 * slots // vols
    scalar = lambda x: jnp.asarray(x, jnp.int32).reshape(1)
    tiles = slot_tile.reshape(slots // LANES, LANES)
    slot = entry_slot.reshape(entries // LANES, LANES)
    factors = [x.reshape(entries // LANES, LANES) for x in (pressure, velocity)]
    core = scalar(pix & 1)
    owners = lax.dynamic_slice_in_dim(
        tile_owner.reshape(vols, block // LANES, LANES), vol, 1
    )[0]
    rows = owned_rows(scalar(pix), owners, most_owned)[0]
    pairs = [(p, p ^ 1) for p in range(pixs)]

    def exchange(cap):
        place, ends, head = plan(scalar(vol), tiles, slot, vols, block, cap)
        place, ends = place.reshape(-1), ends.reshape(-1)
        arrived = []
        names = rows
        for channel, factor in enumerate(factors):
            if channel:
                factor, names = lax.optimization_barrier((factor, names))
            buckets = project(kernel, factor, slot, ends, place, head, vols, cap)
            if channel:
                arrived[0][0], *buckets = lax.optimization_barrier((arrived[0][0], *buckets))
            moved = {0: buckets[0]}
            for k in reversed(range(1, vols)):
                moved[k] = lax.ppermute(buckets[k], "vol", [(d, d ^ k) for d in range(vols)])
            arrived.append([moved[k] for k in range(vols)])
        half = vols // 2
        (near0, far0), (near1, far1) = [(a[:half], a[half:]) for a in arrived]

        def core_sum(near, far, held):
            if held is None:
                held = collect(near, None, None, cap, block)
            keep, send = collect(far, held, core, cap, block)
            return keep + lax.ppermute(send, "pix", pairs)

        def pix_sum(mine):
            step = 2
            while step < pixs:
                mine = mine + lax.ppermute(mine, "pix", [(p, p ^ step) for p in range(pixs)])
                step *= 2
            return mine

        mine0 = core_sum(near0, far0, None)
        mine0, near1[0] = lax.optimization_barrier((mine0, near1[0]))
        held1 = collect(near1, None, None, cap, block)
        mine0 = pix_sum(mine0)
        result = finish(0, core, names, mine0, lax.ppermute(mine0, "pix", pairs), ())
        far1[0], *result = lax.optimization_barrier((far1[0], *result))
        mine1 = pix_sum(core_sum(near1, far1, held1))
        result = finish(1, core, names, mine1, lax.ppermute(mine1, "pix", pairs), result)
        return mine0[block // 2, 0] > 0, *result

    result = exchange(most_rows * 23 // 32 // 8 * 8)

    def redo(state):
        unused, *full = exchange(most_rows)
        return jnp.zeros((), bool), *full

    _, owned, shell = lax.while_loop(lambda state: state[0], redo, result)
    return owned, shell


def solution(mesh):
    in_specs = (
        P(("vol", "pix"), None),
        P(("vol", "pix")),
        P(("vol", "pix")),
        P(("vol", "pix"), None),
        P(("vol", "pix"), None),
        P(),
    )
    out_specs = (P(("vol", "pix"), None), P("vol", None))
    return jax.shard_map(shards, mesh=mesh, in_specs=in_specs, out_specs=out_specs, check_vma=False)
```

```python
import functools

import jax
import jax.numpy as jnp
from jax import lax
from jax.experimental import pallas as pl
from jax.experimental.pallas import tpu as pltpu
from jax.sharding import PartitionSpec as P


LANES = 128
HEAD = 8
ROOM = pltpu.CompilerParams(vmem_limit_bytes=16 << 20)
GROUP = 256
WINDOW = 40


SMEM = pl.BlockSpec(memory_space=pltpu.SMEM)
VMEM = pl.BlockSpec(memory_space=pltpu.VMEM)
ANY = pl.BlockSpec(memory_space=pl.ANY)
HBM = pl.BlockSpec(memory_space=pltpu.HBM)


def iota(shape, axis):
    return lax.broadcasted_iota(jnp.int32, shape, axis)


def nt_dot(a, b):
    return lax.dot_general(a, b, (((1,), (1,)), ((), ())), preferred_element_type=jnp.float32)


def dot(a, b):
    return jnp.dot(a, b, preferred_element_type=jnp.float32)


def ones_where(mask):
    return jnp.where(mask, 1.0, 0.0).astype(jnp.bfloat16)


def bytes_of(x):
    return (x >> 8).astype(jnp.float32), (x & 255).astype(jnp.float32)


def running_counts(marks, rows):
    total = marks.shape[0]
    upper = ones_where(iota((LANES, LANES), 0) <= iota((LANES, LANES), 1))
    row, column = iota((total, total), 0), iota((total, total), 1)
    earlier = ones_where((column < row) & (row // rows == column // rows))
    before = dot(earlier, marks).astype(jnp.bfloat16)
    return dot(marks, upper) + dot(before, jnp.ones((LANES, LANES), jnp.bfloat16))


class Room:
    def __init__(self, vols, near, far, pool):
        self.vols, self.near, self.far, self.pool = vols, near, far, pool
        self.half = vols // 2
        self.lists = -(-max(near, far, pool) // LANES)
        self.sizes = [near] * self.half + [far] * self.half + ([pool] if pool else [])
        self.starts = [sum(self.sizes[:k]) for k in range(len(self.sizes) + 1)]


def plan_kernel(room, block, me_ref, tile_ref, slot_ref, place_ref, ends_ref, head_ref):
    vols, half = room.vols, room.half
    lane = iota((HEAD, LANES), 1)
    line = iota((HEAD, LANES), 0)
    slots = slot_ref[...]
    ends = ones_where(((line == 0) & (lane == 0)) | ((line == 1) & (lane == LANES - 1)))
    high, low = bytes_of(slots)
    ends_ref[...] = (
        nt_dot(ends, high.astype(jnp.bfloat16)) * 256.0 + nt_dot(ends, low.astype(jnp.bfloat16))
    ).astype(jnp.int32)

    me = me_ref[0]
    tiles = tile_ref[...]
    rows = tiles.shape[0]
    vol = tiles // block
    marks = jnp.concatenate([jnp.where(vol == i, 1.0, 0.0) for i in range(vols)], axis=0)
    counts = running_counts(marks.astype(jnp.bfloat16), rows) * marks
    place = jnp.zeros((rows, LANES), jnp.float32)
    for i in range(vols):
        place = place + counts[i * rows : (i + 1) * rows]
    place = place.astype(jnp.int32) - 1
    bucket = vol ^ me
    far = bucket >= half
    fits = place < jnp.where(far, room.far, room.near)
    start = jnp.where(far, half * room.near + (bucket - half) * room.far, bucket * room.near)
    target = jnp.where(fits, start + place, room.starts[-1])
    left = jnp.where(fits, 0.0, 1.0)
    if room.pool:
        extra = jnp.where(far, left, 0.0)
        rank = running_counts(extra.astype(jnp.bfloat16), rows).astype(jnp.int32) - 1
        pooled = (extra > 0) & (rank < room.pool)
        target = jnp.where(pooled, room.starts[vols] + rank, target)
        left = jnp.where(pooled, 0.0, left)
    place_ref[...] = target
    spilled = jnp.sum(left, axis=(0, 1), keepdims=True)
    lists = room.lists
    width = lists * LANES
    high, low = bytes_of(tiles - vol * block + 1)
    pool_high, pool_low = bytes_of(tiles + 1)
    ids = jnp.zeros((2 * vols, width), jnp.float32)
    pool_ids = jnp.zeros((HEAD, width), jnp.float32)
    which = iota((vols, LANES), 0)
    for r in range(rows):
        here = (bucket[r : r + 1] == which) & fits[r : r + 1]
        parts = jnp.concatenate(
            [jnp.where(here, high[r : r + 1], 0.0), jnp.where(here, low[r : r + 1], 0.0)], axis=0
        )
        spots = ones_where(iota((width, LANES), 0) == place[r : r + 1])
        ids = ids + nt_dot(parts.astype(jnp.bfloat16), spots)
        if room.pool:
            parts = jnp.where(line == 0, pool_high[r : r + 1], jnp.where(line == 1, pool_low[r : r + 1], 0.0))
            parts = jnp.where(pooled[r : r + 1], parts, 0.0)
            spots = ones_where(iota((width, LANES), 0) == rank[r : r + 1])
            pool_ids = pool_ids + nt_dot(parts.astype(jnp.bfloat16), spots)
    ids = ids[:vols] * 256.0 + ids[vols:] - 1.0
    pool_ids = pool_ids[0:1] * 256.0 + pool_ids[1:2] - 1.0
    for k in range(len(room.sizes)):
        names = ids[k : k + 1] if k < vols else pool_ids
        head = jnp.where(line == lists, jnp.broadcast_to(spilled, (HEAD, LANES)), 0.0)
        for i in range(lists):
            head = jnp.where(line == i, names[:, i * LANES : (i + 1) * LANES], head)
        head_ref[k * HEAD : (k + 1) * HEAD, :] = head


def plan(me, tiles, slot, room, block):
    rows = tiles.shape[0]
    return pl.pallas_call(
        functools.partial(plan_kernel, room, block),
        in_specs=[SMEM, VMEM, VMEM],
        out_specs=[VMEM, VMEM, VMEM],
        out_shape=[
            jax.ShapeDtypeStruct((rows, LANES), jnp.int32),
            jax.ShapeDtypeStruct((HEAD, slot.shape[0]), jnp.int32),
            jax.ShapeDtypeStruct((len(room.sizes) * HEAD, LANES), jnp.float32),
        ],
        compiler_params=ROOM,
        name="plan",
    )(me, tiles, slot)


def project_kernel(steps, room, named, ends_ref, place_ref, kernel_hbm, factor_ref, slot_ref, head_ref, *rest):
    count = len(room.sizes)
    outs, (kernel_ref, partial_ref, stage_ref, factor_s, in_sem) = rest[:count], rest[count:]
    entries, _ = kernel_ref.shape
    part = entries // steps
    groups = part // GROUP
    lines = GROUP // LANES
    slots = place_ref.shape[0]
    total = entries // LANES

    def load(step):
        piece = pl.ds(pl.multiple_of(step * part, part), part)
        return pltpu.make_async_copy(kernel_hbm.at[piece], kernel_ref.at[piece], in_sem.at[step])

    for step in range(steps):
        load(step).start()
    partial_ref[...] = jnp.zeros_like(partial_ref)
    stage_ref[...] = jnp.zeros_like(stage_ref)
    factor_s[...] = factor_ref[...].astype(jnp.float32)
    line = iota((WINDOW, LANES), 0)

    def first(group):
        return ends_ref[group * lines] & -8

    def reach(group):
        return ends_ref[total + group * lines + lines - 1] - first(group)

    def add(group, base):
        row = []
        for r in range(lines):
            at = pl.ds(group * lines + r, 1)
            row.append(jnp.where(line == slot_ref[at, :] - base, factor_s[at, :], 0.0))
        weights = jnp.concatenate(row, axis=1).astype(jnp.bfloat16)
        sums = dot(weights, kernel_ref[pl.ds(pl.multiple_of(group * GROUP, GROUP), GROUP), :])
        partial_ref[pl.ds(pl.multiple_of(base, 8), WINDOW), :] += sums

    def turn(step, most):
        load(step).wait()
        for g in range(groups):
            group = step * groups + g
            add(group, first(group))
            most = jnp.maximum(most, reach(group))
        return most

    most = lax.fori_loop(0, steps, turn, 0)

    @pl.when(most >= WINDOW)
    def _():
        def more(group, carry):
            def again(w, inner):
                add(group, first(group) + w * WINDOW)
                return inner

            return lax.fori_loop(1, reach(group) // WINDOW + 1, again, carry)

        lax.fori_loop(0, steps * groups, more, 0)

    unroll = 16

    def move(i, carry):
        for u in range(unroll):
            s = i * unroll + u
            stage_ref[pl.ds(place_ref[s], 1), :] = partial_ref[pl.ds(s, 1), :]
        return carry

    lax.fori_loop(0, slots // unroll, move, 0)
    for k, size in enumerate(room.sizes):
        outs[k][:size, :] = stage_ref[room.starts[k] : room.starts[k + 1], :]
        if named:
            outs[k][size:, :] = head_ref[k * HEAD : (k + 1) * HEAD, :]


def project(kernel, factor, slot, ends, place, head, room, named):
    entries, pixels = kernel.shape
    slots = place.shape[0]
    steps = 4
    sizes = [size + HEAD * named for size in room.sizes]
    return pl.pallas_call(
        functools.partial(project_kernel, steps, room, named),
        in_specs=[SMEM, SMEM, HBM, VMEM, VMEM, VMEM],
        out_specs=[VMEM] * len(sizes),
        out_shape=[jax.ShapeDtypeStruct((size, pixels), jnp.float32) for size in sizes],
        scratch_shapes=[
            pltpu.VMEM((entries, pixels), kernel.dtype),
            pltpu.VMEM((slots + WINDOW, pixels), jnp.float32),
            pltpu.VMEM((room.starts[-1] + HEAD, pixels), jnp.float32),
            pltpu.VMEM(factor.shape, jnp.float32),
            pltpu.SemaphoreType.DMA((steps,)),
        ],
        compiler_params=ROOM,
        name="project",
    )(ends, place, kernel, factor, slot, head)


def split(x):
    high = x.astype(jnp.bfloat16)
    return high, (x - high.astype(jnp.float32)).astype(jnp.bfloat16)


def collect_kernel(items, lists, first, last, block, arrays, scalars_ref, *refs):
    inputs, refs = refs[:arrays], refs[arrays:]
    held_ref, refs = (None, refs) if first else (refs[0], refs[1:])
    pixels = inputs[0].shape[1]
    outs, rows_s = refs[: 1 + last], refs[1 + last :]
    flag = jnp.zeros((HEAD, pixels), jnp.float32)
    ids = []
    for value, step, head, size, index, pooled in items:
        rows = inputs[value][index * step : index * step + size, :]
        rows_s[len(ids)][...] = jnp.concatenate(split(rows), axis=1)
        at = index * (size + HEAD) + size
        heads = inputs[head][at : at + HEAD, :]
        if not pooled:
            flag = flag + heads[lists : lists + 1]
        names = jnp.concatenate([heads[i : i + 1] for i in range(lists)], axis=1)[:, :size]
        names = names.astype(jnp.int32)
        ids.append(names - scalars_ref[0] * block if pooled else names)
    if held_ref is not None:
        flag = flag + held_ref[block:, :]

    def total(t, rows):
        sums = jnp.zeros((rows, 2 * pixels), jnp.float32)
        for names, values in zip(ids, rows_s):
            sums = sums + dot(ones_where(iota((rows, names.shape[1]), 0) + t == names), values[...])
        sums = sums[:, :pixels] + sums[:, pixels:]
        return sums if held_ref is None else sums + held_ref[t : t + rows, :]

    chunk = 256
    if not last:
        for t in range(0, block, chunk):
            outs[0][t : t + chunk, :] = total(t, chunk)
        outs[0][block:, :] = flag
        return
    keep_ref, send_ref = outs
    lower = scalars_ref[1] == 0
    half = block // 2
    for t in range(0, half, chunk):
        one, two = total(t, chunk), total(t + half, chunk)
        keep_ref[t : t + chunk, :] = jnp.where(lower, one, two)
        send_ref[t : t + chunk, :] = jnp.where(lower, two, one)
    keep_ref[half:, :] = flag
    send_ref[half:, :] = flag


def collect(parts, held, last, scalars, lists, block):
    inputs, items = [], []
    for values, head, size, count, pooled in parts:
        places = []
        for array in (values, head):
            known = [i for i, other in enumerate(inputs) if other is array]
            places.append(known[0] if known else len(inputs))
            if not known:
                inputs.append(array)
        step = values.shape[0] // count
        items += [(places[0], step, places[1], size, i, pooled) for i in range(count)]
    pixels = inputs[0].shape[1]
    args = [scalars, *inputs] + ([] if held is None else [held])
    rows = block // 2 + HEAD if last else block + HEAD
    out = jax.ShapeDtypeStruct((rows, pixels), jnp.float32)
    return pl.pallas_call(
        functools.partial(collect_kernel, tuple(items), lists, held is None, last, block, len(inputs)),
        in_specs=[SMEM] + [VMEM] * (len(args) - 1),
        out_specs=[VMEM] * 2 if last else VMEM,
        out_shape=[out] * 2 if last else out,
        scratch_shapes=[pltpu.VMEM((item[3], 2 * pixels), jnp.bfloat16) for item in items],
        compiler_params=ROOM,
        name="collect_last" if last else "collect",
    )(*args)


def owner_kernel(most, pix_ref, owner_ref, row_ref):
    owners = owner_ref[...]
    rows = owners.shape[0]
    mine = owners == pix_ref[0]
    marks = jnp.where(mine, 1.0, 0.0)
    rank = running_counts(marks.astype(jnp.bfloat16), rows).astype(jnp.int32) - 1
    index = iota((rows, LANES), 0) * LANES + iota((rows, LANES), 1) + 1
    found = jnp.zeros((HEAD, most), jnp.float32)
    part = iota((HEAD, LANES), 0)
    for r in range(rows):
        here = mine[r : r + 1]
        high = jnp.where(here, (index[r : r + 1] // 64).astype(jnp.float32), 0.0)
        low = jnp.where(here, (index[r : r + 1] % 64).astype(jnp.float32), 0.0)
        parts = jnp.where(part == 0, high, jnp.where(part == 1, low, 0.0))
        spots = ones_where(iota((most, LANES), 0) == rank[r : r + 1])
        found = found + nt_dot(parts.astype(jnp.bfloat16), spots)
    tile = (found[0:1] * 64.0 + found[1:2]).astype(jnp.int32) - 1
    tile = jnp.where(tile < 0, rows * LANES, tile)
    row_ref[...] = jnp.broadcast_to(tile, (HEAD, most))


def owned_rows(pix, owners, most):
    return pl.pallas_call(
        functools.partial(owner_kernel, most),
        in_specs=[SMEM, VMEM],
        out_specs=VMEM,
        out_shape=jax.ShapeDtypeStruct((HEAD, most), jnp.int32),
        compiler_params=ROOM,
        name="owned_rows",
    )(pix, owners)


def finish_kernel(channel, core_ref, row_ref, mine_ref, other_ref, *rest):
    owned_ref, map_ref, full_ref, own_ref = rest[-4:]
    half, pixels = mine_ref.shape[0] - HEAD, mine_ref.shape[1]
    columns = slice(channel * pixels, (channel + 1) * pixels)
    core = core_ref[0]
    for at, part in ((core, mine_ref), (1 - core, other_ref)):
        at = pl.ds(pl.multiple_of(at * half, half), half)
        value = part[:half, :]
        full_ref[at, :] = value
        map_ref[at, columns] = value
    full_ref[2 * half :, :] = jnp.zeros((HEAD, pixels), jnp.float32)
    unroll = 16

    def move(i, carry):
        for u in range(unroll):
            r = i * unroll + u
            own_ref[pl.ds(r, 1), :] = full_ref[pl.ds(row_ref[r], 1), :]
        return carry

    lax.fori_loop(0, own_ref.shape[0] // unroll, move, 0)
    owned_ref[:, columns] = own_ref[...]


def finish(channel, core, rows, mine, other, before):
    block, pixels = 2 * (mine.shape[0] - HEAD), mine.shape[1]
    return pl.pallas_call(
        functools.partial(finish_kernel, channel),
        in_specs=[SMEM, SMEM, VMEM, VMEM] + [VMEM] * len(before),
        out_specs=[VMEM, VMEM],
        out_shape=[
            jax.ShapeDtypeStruct((rows.shape[0], 2 * pixels), jnp.float32),
            jax.ShapeDtypeStruct((block, 2 * pixels), jnp.float32),
        ],
        input_output_aliases={4: 0, 5: 1} if before else {},
        scratch_shapes=[
            pltpu.VMEM((block + HEAD, pixels), jnp.float32),
            pltpu.VMEM((rows.shape[0], pixels), jnp.float32),
        ],
        compiler_params=ROOM,
        name="finish",
    )(core, rows, mine, other, *before)


def shards(kernel, pressure, velocity, entry_slot, slot_tile, tile_owner):
    vols = lax.axis_size("vol")
    pixs = lax.axis_size("pix")
    vol = lax.axis_index("vol")
    pix = lax.axis_index("pix")
    entries, _ = kernel.shape
    slots = slot_tile.shape[1]
    block = tile_owner.shape[0] // vols
    most_owned = 2 * block // pixs
    most_rows = 2 * slots // vols
    scalar = lambda x: jnp.asarray(x, jnp.int32).reshape(1)
    tiles = slot_tile.reshape(slots // LANES, LANES)
    slot = entry_slot.reshape(entries // LANES, LANES)
    factors = [x.reshape(entries // LANES, LANES) for x in (pressure, velocity)]
    core = scalar(pix & 1)
    owners = lax.dynamic_slice_in_dim(
        tile_owner.reshape(vols, block // LANES, LANES), vol, 1
    )[0]
    rows = owned_rows(scalar(pix), owners, most_owned)[0]
    pairs = [(p, p ^ 1) for p in range(pixs)]

    scalars = jnp.stack([vol, pix & 1]).astype(jnp.int32)
    hops = [1 << i for i in reversed(range((vols // 2).bit_length() - 1))]

    def send(x, k):
        return lax.ppermute(x, "vol", [(d, d ^ k) for d in range(vols)])

    def exchange(room):
        place, ends, head = plan(scalar(vol), tiles, slot, room, block)
        place, ends = place.reshape(-1), ends.reshape(-1)
        half = vols // 2
        arrived, pools = [], []
        names = rows
        for channel, factor in enumerate(factors):
            if channel:
                factor, names = lax.optimization_barrier((factor, names))
            parts = project(kernel, factor, slot, ends, place, head, room, channel == 0)
            if channel:
                arrived[0][0], *parts = lax.optimization_barrier((arrived[0][0], *parts))
            if room.pool:
                pool = send(parts[vols], half)
                if channel:
                    parts[0], pools[0] = lax.optimization_barrier((parts[0], pools[0]))
                pools.append(pool)
            moved = {0: parts[0]}
            for k in reversed(range(1, vols)):
                moved[k] = send(parts[k], k)
            arrived.append([moved[k] for k in range(vols)])

        def spread(channel):
            pool = pools[channel]
            for k in hops:
                pool = jnp.concatenate([pool, send(pool, k)], axis=0)
            return pool

        heads = arrived[0]
        if room.pool:
            pools[0] = spread(0)
            pools[1] = spread(1)

        def near(channel):
            parts = [(arrived[channel][k], heads[k], room.near, 1, False) for k in range(half)]
            return collect(parts, None, False, scalars, room.lists, block)

        def core_sum(channel, held):
            parts = [(arrived[channel][k], heads[k], room.far, 1, False) for k in range(half, vols)]
            if room.pool:
                parts.append((pools[channel], pools[0], room.pool, half, True))
            keep, give = collect(parts, held, True, scalars, room.lists, block)
            return keep + lax.ppermute(give, "pix", pairs)

        def pix_sum(mine):
            step = 2
            while step < pixs:
                mine = mine + lax.ppermute(mine, "pix", [(p, p ^ step) for p in range(pixs)])
                step *= 2
            return mine

        mine0 = core_sum(0, near(0))
        mine0, arrived[1][0] = lax.optimization_barrier((mine0, arrived[1][0]))
        held1 = near(1)
        mine0 = pix_sum(mine0)
        mine0, arrived[1][half] = lax.optimization_barrier((mine0, arrived[1][half]))
        result = finish(0, core, names, mine0, lax.ppermute(mine0, "pix", pairs), ())
        mine1 = pix_sum(core_sum(1, held1))
        result = finish(1, core, names, mine1, lax.ppermute(mine1, "pix", pairs), result)
        return mine0[block // 2, 0] > 0, *result

    def rows_of(share):
        return most_rows * share // 32 // 8 * 8

    result = exchange(Room(vols, rows_of(23), rows_of(17), rows_of(6)))

    def redo(state):
        unused, *full = exchange(Room(vols, most_rows, most_rows, 0))
        return jnp.zeros((), bool), *full

    _, owned, shell = lax.while_loop(lambda state: state[0], redo, result)
    return owned, shell


def solution(mesh):
    in_specs = (
        P(("vol", "pix"), None),
        P(("vol", "pix")),
        P(("vol", "pix")),
        P(("vol", "pix"), None),
        P(("vol", "pix"), None),
        P(),
    )
    out_specs = (P(("vol", "pix"), None), P("vol", None))
    return jax.shard_map(shards, mesh=mesh, in_specs=in_specs, out_specs=out_specs, check_vma=False)
```

```python
import functools

import jax
import jax.numpy as jnp
from jax import lax
from jax.experimental import pallas as pl
from jax.experimental.pallas import tpu as pltpu
from jax.sharding import PartitionSpec as P


LANES = 128
HEAD = 8
ROOM = pltpu.CompilerParams(vmem_limit_bytes=16 << 20)
GROUP = 256
WINDOW = 40


SMEM = pl.BlockSpec(memory_space=pltpu.SMEM)
VMEM = pl.BlockSpec(memory_space=pltpu.VMEM)
ANY = pl.BlockSpec(memory_space=pl.ANY)
HBM = pl.BlockSpec(memory_space=pltpu.HBM)


def iota(shape, axis):
    return lax.broadcasted_iota(jnp.int32, shape, axis)


def nt_dot(a, b):
    return lax.dot_general(a, b, (((1,), (1,)), ((), ())), preferred_element_type=jnp.float32)


def dot(a, b):
    return jnp.dot(a, b, preferred_element_type=jnp.float32)


def ones_where(mask):
    return jnp.where(mask, 1.0, 0.0).astype(jnp.bfloat16)


def bytes_of(x):
    return (x >> 8).astype(jnp.float32), (x & 255).astype(jnp.float32)


def running_counts(marks, rows):
    total = marks.shape[0]
    upper = ones_where(iota((LANES, LANES), 0) <= iota((LANES, LANES), 1))
    row, column = iota((total, total), 0), iota((total, total), 1)
    earlier = ones_where((column < row) & (row // rows == column // rows))
    before = dot(earlier, marks).astype(jnp.bfloat16)
    return dot(marks, upper) + dot(before, jnp.ones((LANES, LANES), jnp.bfloat16))


def plan_kernel(vols, parts, block, cap, me_ref, tile_ref, slot_ref, place_ref, ends_ref, head_ref):
    size = cap + HEAD
    part_tiles = block // parts
    lane = iota((HEAD, LANES), 1)
    line = iota((HEAD, LANES), 0)
    slots = slot_ref[...]
    ends = ones_where(((line == 0) & (lane == 0)) | ((line == 1) & (lane == LANES - 1)))
    high, low = bytes_of(slots)
    ends_ref[...] = (
        nt_dot(ends, high.astype(jnp.bfloat16)) * 256.0 + nt_dot(ends, low.astype(jnp.bfloat16))
    ).astype(jnp.int32)

    tiles = tile_ref[...]
    rows = tiles.shape[0]
    classes = vols * parts
    part = tiles // part_tiles
    group = part ^ (me_ref[0] * parts + me_ref[1])
    marks = jnp.concatenate([jnp.where(group == i, 1.0, 0.0) for i in range(classes)], axis=0)
    counts = running_counts(marks.astype(jnp.bfloat16), rows) * marks
    place = jnp.zeros((rows, LANES), jnp.float32)
    for i in range(classes):
        place = place + counts[i * rows : (i + 1) * rows]
    place = place.astype(jnp.int32) - 1
    fits = place < cap
    place_ref[...] = jnp.where(fits, group * size + place, classes * size)
    spilled = jnp.sum(jnp.where(fits, 0.0, 1.0), axis=(0, 1), keepdims=True)
    lists = -(-2 * size // LANES)
    width = lists * LANES
    spot = jnp.where(fits, place + me_ref[2] * size, -1)
    high, low = bytes_of(tiles - part * part_tiles + 1)
    ids = jnp.zeros((2 * classes, width), jnp.float32)
    which = iota((classes, LANES), 0)
    for r in range(rows):
        here = group[r : r + 1] == which
        pieces = jnp.concatenate(
            [jnp.where(here, high[r : r + 1], 0.0), jnp.where(here, low[r : r + 1], 0.0)], axis=0
        )
        spots = ones_where(iota((width, LANES), 0) == spot[r : r + 1])
        ids = ids + nt_dot(pieces.astype(jnp.bfloat16), spots)
    ids = ids[:classes] * 256.0 + ids[classes:]
    for k in range(classes):
        head = jnp.where(line == lists, jnp.broadcast_to(spilled, (HEAD, LANES)), 0.0)
        for i in range(lists):
            head = jnp.where(line == i, ids[k : k + 1, i * LANES : (i + 1) * LANES], head)
        head_ref[k * HEAD : (k + 1) * HEAD, :] = head


def plan(me, tiles, slot, vols, parts, block, cap):
    rows = tiles.shape[0]
    return pl.pallas_call(
        functools.partial(plan_kernel, vols, parts, block, cap),
        in_specs=[SMEM, VMEM, VMEM],
        out_specs=[VMEM, VMEM, VMEM],
        out_shape=[
            jax.ShapeDtypeStruct((rows, LANES), jnp.int32),
            jax.ShapeDtypeStruct((HEAD, slot.shape[0]), jnp.int32),
            jax.ShapeDtypeStruct((vols * parts * HEAD, LANES), jnp.float32),
        ],
        compiler_params=ROOM,
        name="plan",
    )(me, tiles, slot)


def project_kernel(
    steps, cap, own, me_ref, ends_ref, place_ref, kernel_hbm, thermal_ref, kinetic_ref, slot_ref, head_ref,
    out_ref, kernel_ref, partial_ref, stage_ref, factor_s, in_sem
):
    entries, _ = kernel_ref.shape
    part = entries // steps
    groups = part // GROUP
    lines = GROUP // LANES
    slots = place_ref.shape[0]
    total = entries // LANES

    def load(step):
        piece = pl.ds(pl.multiple_of(step * part, part), part)
        return pltpu.make_async_copy(kernel_hbm.at[piece], kernel_ref.at[piece], in_sem.at[step])

    for step in range(steps):
        load(step).start()
    partial_ref[...] = jnp.zeros_like(partial_ref)
    stage_ref[...] = jnp.zeros_like(stage_ref)
    first_channel = (me_ref[2] == 0) == own
    factor_s[...] = jnp.where(first_channel, thermal_ref[...].astype(jnp.float32), kinetic_ref[...].astype(jnp.float32))
    line = iota((WINDOW, LANES), 0)

    def first(group):
        return ends_ref[group * lines] & -8

    def reach(group):
        return ends_ref[total + group * lines + lines - 1] - first(group)

    def add(group, base):
        row = []
        for r in range(lines):
            at = pl.ds(group * lines + r, 1)
            row.append(jnp.where(line == slot_ref[at, :] - base, factor_s[at, :], 0.0))
        weights = jnp.concatenate(row, axis=1).astype(jnp.bfloat16)
        sums = dot(weights, kernel_ref[pl.ds(pl.multiple_of(group * GROUP, GROUP), GROUP), :])
        partial_ref[pl.ds(pl.multiple_of(base, 8), WINDOW), :] += sums

    def turn(step, most):
        load(step).wait()
        for g in range(groups):
            group = step * groups + g
            add(group, first(group))
            most = jnp.maximum(most, reach(group))
        return most

    most = lax.fori_loop(0, steps, turn, 0)

    @pl.when(most >= WINDOW)
    def _():
        def more(group, carry):
            def again(w, inner):
                add(group, first(group) + w * WINDOW)
                return inner

            return lax.fori_loop(1, reach(group) // WINDOW + 1, again, carry)

        lax.fori_loop(0, steps * groups, more, 0)

    unroll = 16

    def move(i, carry):
        for u in range(unroll):
            s = i * unroll + u
            stage_ref[pl.ds(place_ref[s], 1), :] = partial_ref[pl.ds(s, 1), :]
        return carry

    lax.fori_loop(0, slots // unroll, move, 0)
    size = cap + HEAD
    for k in range(head_ref.shape[0] // HEAD):
        out_ref[k * size : k * size + cap, :] = stage_ref[k * size : k * size + cap, :]
        out_ref[k * size + cap : (k + 1) * size, :] = head_ref[k * HEAD : (k + 1) * HEAD, :]


def project(me, kernel, factors, slot, ends, place, head, cap, own):
    entries, pixels = kernel.shape
    slots = place.shape[0]
    steps = 4
    rows = head.shape[0] // HEAD * (cap + HEAD)
    return pl.pallas_call(
        functools.partial(project_kernel, steps, cap, own),
        in_specs=[SMEM, SMEM, SMEM, HBM, VMEM, VMEM, VMEM, VMEM],
        out_specs=VMEM,
        out_shape=jax.ShapeDtypeStruct((rows, pixels), jnp.float32),
        scratch_shapes=[
            pltpu.VMEM((entries, pixels), kernel.dtype),
            pltpu.VMEM((slots + WINDOW, pixels), jnp.float32),
            pltpu.VMEM((rows + HEAD, pixels), jnp.float32),
            pltpu.VMEM(slot.shape, jnp.float32),
            pltpu.SemaphoreType.DMA((steps,)),
        ],
        compiler_params=ROOM,
        name="project",
    )(me, ends, place, kernel, *factors, slot, head)


def pack_kernel(first, size, me_ref, mine_ref, other_ref, *outs):
    core = me_ref[2]
    for at, rows in ((core, mine_ref), (1 - core, other_ref)):
        at = pl.ds(pl.multiple_of(at * size, 8), size)
        for k, out in enumerate(outs):
            out[at, :] = rows[(first + k) * size : (first + k + 1) * size, :]


def pack(me, mine, other, first, count, size):
    out = jax.ShapeDtypeStruct((2 * size, mine.shape[1]), jnp.float32)
    return pl.pallas_call(
        functools.partial(pack_kernel, first, size),
        in_specs=[SMEM, VMEM, VMEM],
        out_specs=[VMEM] * count,
        out_shape=[out] * count,
        compiler_params=ROOM,
        name="pack",
    )(me, mine, other)


def split(x):
    high = x.astype(jnp.bfloat16)
    return high, (x - high.astype(jnp.float32)).astype(jnp.bfloat16)


def collect_kernel(size, part_tiles, *refs):
    messages, (out_ref, *rows_s) = refs[: len(refs) // 2], refs[len(refs) // 2 :]
    pixels = out_ref.shape[1]
    lists = -(-2 * size // LANES)
    flag = jnp.zeros((HEAD, pixels), jnp.float32)
    ids = []
    for message, rows in zip(messages, rows_s):
        rows[...] = jnp.concatenate(split(message[...]), axis=1)
        head = message[size - HEAD : size, :] + message[2 * size - HEAD : 2 * size, :]
        flag = flag + head[lists : lists + 1]
        names = jnp.concatenate([head[i : i + 1] for i in range(lists)], axis=1)[:, : 2 * size]
        ids.append(names.astype(jnp.int32) - 1)
    chunk = min(256, part_tiles)
    for t in range(0, part_tiles, chunk):
        sums = jnp.zeros((chunk, 2 * pixels), jnp.float32)
        for names, rows in zip(ids, rows_s):
            sums = sums + dot(ones_where(iota((chunk, 2 * size), 0) + t == names), rows[...])
        out_ref[t : t + chunk, :] = sums[:, :pixels] + sums[:, pixels:]
    out_ref[part_tiles:, :] = flag


def collect(messages, part_tiles):
    rows, pixels = messages[0].shape
    return pl.pallas_call(
        functools.partial(collect_kernel, rows // 2, part_tiles),
        in_specs=[VMEM] * len(messages),
        out_specs=VMEM,
        out_shape=jax.ShapeDtypeStruct((part_tiles + HEAD, pixels), jnp.float32),
        scratch_shapes=[pltpu.VMEM((rows, 2 * pixels), jnp.bfloat16)] * len(messages),
        compiler_params=ROOM,
        name="collect",
    )(*messages)


def owner_kernel(parts, me_ref, owner_ref, row_ref):
    most = row_ref.shape[1]
    owners = owner_ref[...]
    rows = owners.shape[0]
    mine = owners == me_ref[1] * 2 + me_ref[2]
    marks = jnp.where(mine, 1.0, 0.0)
    rank = running_counts(marks.astype(jnp.bfloat16), rows).astype(jnp.int32) - 1
    index = iota((rows, LANES), 0) * LANES + iota((rows, LANES), 1)
    found = jnp.zeros((HEAD, most), jnp.float32)
    line = iota((HEAD, LANES), 0)
    high, low = bytes_of(index + 1)
    for r in range(rows):
        pieces = jnp.where(line == 0, high[r : r + 1], jnp.where(line == 1, low[r : r + 1], 0.0))
        pieces = jnp.where(mine[r : r + 1], pieces, 0.0)
        spots = ones_where(iota((most, LANES), 0) == rank[r : r + 1])
        found = found + nt_dot(pieces.astype(jnp.bfloat16), spots)
    tile = (found[0:1] * 256.0 + found[1:2]).astype(jnp.int32) - 1
    tile = jnp.where(tile < 0, rows * LANES, tile)
    bounds = jnp.zeros((1, most), jnp.float32)
    for p in range(1, parts + 1):
        before = jnp.where(index < p * (rows * LANES // parts), marks, 0.0)
        bounds = jnp.where(iota((1, most), 1) == p, jnp.sum(before, axis=(0, 1), keepdims=True), bounds)
    row_ref[...] = jnp.where(iota((HEAD, most), 0) == 0, tile, bounds.astype(jnp.int32))


def owned_rows(me, owners, most, parts):
    return pl.pallas_call(
        functools.partial(owner_kernel, parts),
        in_specs=[SMEM, VMEM],
        out_specs=VMEM,
        out_shape=jax.ShapeDtypeStruct((HEAD, most), jnp.int32),
        compiler_params=ROOM,
        name="owned_rows",
    )(me, owners)


def fill_rows(row_ref, table_ref, owned_ref, start, end):
    unroll = 8

    def one(r):
        owned_ref[pl.ds(r, 1), :] = table_ref[pl.ds(row_ref[r], 1), :]

    def group(i, carry):
        for u in range(unroll):
            one(start + i * unroll + u)
        return carry

    def rest(r, carry):
        one(r)
        return carry

    groups = (end - start) // unroll
    lax.fori_loop(0, groups, group, 0)
    lax.fori_loop(start + groups * unroll, end, rest, 0)


def place_part(m, part_tiles, me_ref, own_ref, other_ref, map_ref):
    pixels = own_ref.shape[1]
    own, other = own_ref[:part_tiles, :], other_ref[:part_tiles, :]
    at = pl.ds(pl.multiple_of((me_ref[1] ^ m) * part_tiles, part_tiles), part_tiles)
    map_ref[at, :pixels] = jnp.where(me_ref[2] == 0, own, other)
    map_ref[at, pixels:] = jnp.where(me_ref[2] == 0, other, own)


def early_kernel(parts, me_ref, row_ref, own_ref, other_ref, owned_ref, map_ref):
    most = owned_ref.shape[0]
    owned_ref[...] = jnp.zeros_like(owned_ref)
    place_part(0, map_ref.shape[0] // parts, me_ref, own_ref, other_ref, map_ref)
    x = me_ref[1]
    fill_rows(row_ref, map_ref, owned_ref, row_ref[most + x], row_ref[most + x + 1])


def late_kernel(parts, me_ref, row_ref, *refs):
    pieces, (early_owned, early_map, owned_ref, map_ref) = refs[:-4], refs[-4:]
    most = owned_ref.shape[0]
    part_tiles = map_ref.shape[0] // parts
    x = me_ref[1]
    mine = pl.ds(pl.multiple_of(x * part_tiles, part_tiles), part_tiles)
    owned_ref[...] = early_owned[...]
    map_ref[mine, :] = early_map[mine, :]
    for m in range(1, parts):
        place_part(m, part_tiles, me_ref, pieces[2 * m - 2], pieces[2 * m - 1], map_ref)
    fill_rows(row_ref, map_ref, owned_ref, 0, row_ref[most + x])
    fill_rows(row_ref, map_ref, owned_ref, row_ref[most + x + 1], row_ref[most + parts])


def finish(kernel, me, rows, pieces, most, block, parts):
    width = 2 * pieces[0].shape[1]
    return pl.pallas_call(
        functools.partial(kernel, parts),
        in_specs=[SMEM, SMEM] + [VMEM] * len(pieces),
        out_specs=[VMEM, VMEM],
        out_shape=[
            jax.ShapeDtypeStruct((most, width), jnp.float32),
            jax.ShapeDtypeStruct((block, width), jnp.float32),
        ],
        compiler_params=ROOM,
    )(me, rows, *pieces)


def shards(kernel, pressure, velocity, entry_slot, slot_tile, tile_owner):
    vols = lax.axis_size("vol")
    pixs = lax.axis_size("pix")
    vol = lax.axis_index("vol")
    pix = lax.axis_index("pix")
    entries, _ = kernel.shape
    slots = slot_tile.shape[1]
    block = tile_owner.shape[0] // vols
    parts = pixs // 2
    part_tiles = block // parts
    half = vols // 2
    most_owned = 2 * block // pixs
    most_rows = min(2 * slots // vols, part_tiles)
    me = jnp.stack([vol, pix >> 1, pix & 1]).astype(jnp.int32)
    tiles = slot_tile.reshape(slots // LANES, LANES)
    slot = entry_slot.reshape(entries // LANES, LANES)
    factors = [x.reshape(entries // LANES, LANES) for x in (pressure, velocity)]
    owners = lax.dynamic_slice_in_dim(
        tile_owner.reshape(vols, block // LANES, LANES), vol, 1
    )[0]
    rows = owned_rows(me, owners, most_owned, parts)[:2].reshape(-1)

    def send(x, vol_step=0, part_step=0, core_step=0):
        step = (vol_step * parts + part_step) * 2 + core_step
        return lax.ppermute(x, ("vol", "pix"), [(d, d ^ step) for d in range(vols * pixs)])

    def exchange(cap):
        size = cap + HEAD
        count = half * parts
        place, ends, head = plan(me, tiles, slot, vols, parts, block, cap)
        place, ends = place.reshape(-1), ends.reshape(-1)
        given = project(me, kernel, factors, slot, ends, place, head, cap, False)
        taken = send(given, core_step=1)
        held = project(me, kernel, factors, slot, ends, place, head, cap, True)

        def gather(first):
            messages = list(pack(me, held, taken, first, count, size))
            for k in reversed(range(1, count)):
                messages[k] = send(messages[k], k // parts, k % parts)
            return collect(messages, part_tiles)

        far = send(gather(count), vol_step=half)
        mine = gather(0) + far
        other = send(mine, core_step=1)
        early = finish(early_kernel, me, rows, [mine, other], most_owned, block, parts)
        pieces = []
        for m in range(1, parts):
            piece = send(mine, part_step=m)
            pieces += [piece, send(piece, core_step=1)]
        full = finish(late_kernel, me, rows, [*pieces, *early], most_owned, block, parts)
        return mine[part_tiles, 0] > 0, *full

    result = exchange(most_rows * 13 // 32 // 8 * 8)

    def redo(state):
        unused, *full = exchange(most_rows)
        return jnp.zeros((), bool), *full

    _, owned, shell = lax.while_loop(lambda state: state[0], redo, result)
    return owned, shell


def solution(mesh):
    in_specs = (
        P(("vol", "pix"), None),
        P(("vol", "pix")),
        P(("vol", "pix")),
        P(("vol", "pix"), None),
        P(("vol", "pix"), None),
        P(),
    )
    out_specs = (P(("vol", "pix"), None), P("vol", None))
    return jax.shard_map(shards, mesh=mesh, in_specs=in_specs, out_specs=out_specs, check_vma=False)
```

```python
import functools

import jax
import jax.numpy as jnp
from jax import lax
from jax.experimental import pallas as pl
from jax.experimental.pallas import tpu as pltpu
from jax.sharding import PartitionSpec as P


LANES = 128
HEAD = 8
ROOM = pltpu.CompilerParams(vmem_limit_bytes=16 << 20)
GROUP = 256
WINDOW = 40


SMEM = pl.BlockSpec(memory_space=pltpu.SMEM)
VMEM = pl.BlockSpec(memory_space=pltpu.VMEM)
ANY = pl.BlockSpec(memory_space=pl.ANY)
HBM = pl.BlockSpec(memory_space=pltpu.HBM)


def iota(shape, axis):
    return lax.broadcasted_iota(jnp.int32, shape, axis)


def nt_dot(a, b):
    return lax.dot_general(a, b, (((1,), (1,)), ((), ())), preferred_element_type=jnp.float32)


def dot(a, b):
    return jnp.dot(a, b, preferred_element_type=jnp.float32)


def ones_where(mask):
    return jnp.where(mask, 1.0, 0.0).astype(jnp.bfloat16)


def bytes_of(x):
    return (x >> 8).astype(jnp.float32), (x & 255).astype(jnp.float32)


def running_counts(marks, rows):
    total = marks.shape[0]
    upper = ones_where(iota((LANES, LANES), 0) <= iota((LANES, LANES), 1))
    row, column = iota((total, total), 0), iota((total, total), 1)
    earlier = ones_where((column < row) & (row // rows == column // rows))
    before = dot(earlier, marks).astype(jnp.bfloat16)
    return dot(marks, upper) + dot(before, jnp.ones((LANES, LANES), jnp.bfloat16))


def plan_kernel(vols, parts, block, cap, me_ref, tile_ref, slot_ref, place_ref, ends_ref, head_ref):
    size = cap + HEAD
    part_tiles = block // parts
    lane = iota((HEAD, LANES), 1)
    line = iota((HEAD, LANES), 0)
    slots = slot_ref[...]
    ends = ones_where(((line == 0) & (lane == 0)) | ((line == 1) & (lane == LANES - 1)))
    high, low = bytes_of(slots)
    ends_ref[...] = (
        nt_dot(ends, high.astype(jnp.bfloat16)) * 256.0 + nt_dot(ends, low.astype(jnp.bfloat16))
    ).astype(jnp.int32)

    tiles = tile_ref[...]
    rows = tiles.shape[0]
    classes = vols * parts
    part = tiles // part_tiles
    group = part ^ (me_ref[0] * parts + me_ref[1])
    marks = jnp.concatenate([jnp.where(group == i, 1.0, 0.0) for i in range(classes)], axis=0)
    counts = running_counts(marks.astype(jnp.bfloat16), rows) * marks
    place = jnp.zeros((rows, LANES), jnp.float32)
    for i in range(classes):
        place = place + counts[i * rows : (i + 1) * rows]
    place = place.astype(jnp.int32) - 1
    fits = place < cap
    place_ref[...] = jnp.where(fits, group * size + place, classes * size)
    spilled = jnp.sum(jnp.where(fits, 0.0, 1.0), axis=(0, 1), keepdims=True)
    lists = -(-2 * size // LANES)
    width = lists * LANES
    spot = jnp.where(fits, place + me_ref[2] * size, -1)
    high, low = bytes_of(tiles - part * part_tiles + 1)
    ids = jnp.zeros((2 * classes, width), jnp.float32)
    which = iota((classes, LANES), 0)
    for r in range(rows):
        here = group[r : r + 1] == which
        pieces = jnp.concatenate(
            [jnp.where(here, high[r : r + 1], 0.0), jnp.where(here, low[r : r + 1], 0.0)], axis=0
        )
        spots = ones_where(iota((width, LANES), 0) == spot[r : r + 1])
        ids = ids + nt_dot(pieces.astype(jnp.bfloat16), spots)
    ids = ids[:classes] * 256.0 + ids[classes:]
    for k in range(classes):
        head = jnp.where(line == lists, jnp.broadcast_to(spilled, (HEAD, LANES)), 0.0)
        for i in range(lists):
            head = jnp.where(line == i, ids[k : k + 1, i * LANES : (i + 1) * LANES], head)
        head_ref[k * HEAD : (k + 1) * HEAD, :] = head


def plan(me, tiles, slot, vols, parts, block, cap):
    rows = tiles.shape[0]
    return pl.pallas_call(
        functools.partial(plan_kernel, vols, parts, block, cap),
        in_specs=[SMEM, VMEM, VMEM],
        out_specs=[VMEM, VMEM, VMEM],
        out_shape=[
            jax.ShapeDtypeStruct((rows, LANES), jnp.int32),
            jax.ShapeDtypeStruct((HEAD, slot.shape[0]), jnp.int32),
            jax.ShapeDtypeStruct((vols * parts * HEAD, LANES), jnp.float32),
        ],
        compiler_params=ROOM,
        name="plan",
    )(me, tiles, slot)


def project_kernel(
    steps, cap, me_ref, ends_ref, place_ref, kernel_hbm, thermal_ref, kinetic_ref, slot_ref, head_ref,
    far_own_ref, near_own_ref, far_other_ref, near_other_ref,
    kernel_ref, own_ref, other_ref, own_stage, other_stage, own_s, other_s, in_sem
):
    entries, _ = kernel_ref.shape
    part = entries // steps
    groups = part // GROUP
    lines = GROUP // LANES
    slots = place_ref.shape[0]
    total = entries // LANES

    def load(step):
        piece = pl.ds(pl.multiple_of(step * part, part), part)
        return pltpu.make_async_copy(kernel_hbm.at[piece], kernel_ref.at[piece], in_sem.at[step])

    for step in range(steps):
        load(step).start()
    for ref in (own_ref, other_ref, own_stage, other_stage):
        ref[...] = jnp.zeros_like(ref)
    thermal, kinetic = thermal_ref[...].astype(jnp.float32), kinetic_ref[...].astype(jnp.float32)
    own_s[...] = jnp.where(me_ref[2] == 0, thermal, kinetic)
    other_s[...] = jnp.where(me_ref[2] == 0, kinetic, thermal)
    line = iota((WINDOW, LANES), 0)

    def first(group):
        return ends_ref[group * lines] & -8

    def reach(group):
        return ends_ref[total + group * lines + lines - 1] - first(group)

    def add(group, base):
        own, other = [], []
        for r in range(lines):
            at = pl.ds(group * lines + r, 1)
            match = line == slot_ref[at, :] - base
            own.append(jnp.where(match, own_s[at, :], 0.0))
            other.append(jnp.where(match, other_s[at, :], 0.0))
        weights = jnp.concatenate(
            [jnp.concatenate(own, axis=1), jnp.concatenate(other, axis=1)], axis=0
        ).astype(jnp.bfloat16)
        sums = dot(weights, kernel_ref[pl.ds(pl.multiple_of(group * GROUP, GROUP), GROUP), :])
        window = pl.ds(pl.multiple_of(base, 8), WINDOW)
        own_ref[window, :] += sums[:WINDOW]
        other_ref[window, :] += sums[WINDOW:]

    def turn(step, most):
        load(step).wait()
        for g in range(groups):
            group = step * groups + g
            add(group, first(group))
            most = jnp.maximum(most, reach(group))
        return most

    most = lax.fori_loop(0, steps, turn, 0)

    @pl.when(most >= WINDOW)
    def _():
        def more(group, carry):
            def again(w, inner):
                add(group, first(group) + w * WINDOW)
                return inner

            return lax.fori_loop(1, reach(group) // WINDOW + 1, again, carry)

        lax.fori_loop(0, steps * groups, more, 0)

    unroll = 16

    def move(i, carry):
        for u in range(unroll):
            s = i * unroll + u
            to = place_ref[s]
            own_stage[pl.ds(to, 1), :] = own_ref[pl.ds(s, 1), :]
            other_stage[pl.ds(to, 1), :] = other_ref[pl.ds(s, 1), :]
        return carry

    lax.fori_loop(0, slots // unroll, move, 0)
    size = cap + HEAD
    classes = head_ref.shape[0] // HEAD
    count = classes // 2
    for near, far, stage in ((near_own_ref, far_own_ref, own_stage), (near_other_ref, far_other_ref, other_stage)):
        for k in range(classes):
            out, at = (near, k * size) if k < count else (far, (k - count) * size)
            out[at : at + cap, :] = stage[k * size : k * size + cap, :]
            out[at + cap : at + size, :] = head_ref[k * HEAD : (k + 1) * HEAD, :]


def project(me, kernel, factors, slot, ends, place, head, cap):
    entries, pixels = kernel.shape
    slots = place.shape[0]
    steps = 4
    rows = head.shape[0] // HEAD * (cap + HEAD)
    partial = pltpu.VMEM((slots + WINDOW, pixels), jnp.float32)
    stage = pltpu.VMEM((rows + HEAD, pixels), jnp.float32)
    factor = pltpu.VMEM(slot.shape, jnp.float32)
    return pl.pallas_call(
        functools.partial(project_kernel, steps, cap),
        in_specs=[SMEM, SMEM, SMEM, HBM, VMEM, VMEM, VMEM, VMEM],
        out_specs=[VMEM] * 4,
        out_shape=[jax.ShapeDtypeStruct((rows // 2, pixels), jnp.float32)] * 4,
        scratch_shapes=[
            pltpu.VMEM((entries, pixels), kernel.dtype),
            partial, partial, stage, stage, factor, factor,
            pltpu.SemaphoreType.DMA((steps,)),
        ],
        compiler_params=ROOM,
        name="project",
    )(me, ends, place, kernel, *factors, slot, head)


def pack_kernel(size, me_ref, mine_ref, other_ref, *outs):
    core = me_ref[2]
    for at, rows in ((core, mine_ref), (1 - core, other_ref)):
        at = pl.ds(pl.multiple_of(at * size, 8), size)
        for k, out in enumerate(outs):
            out[at, :] = rows[k * size : (k + 1) * size, :]


def pack(me, mine, other, size):
    count = mine.shape[0] // size
    out = jax.ShapeDtypeStruct((2 * size, mine.shape[1]), jnp.float32)
    return pl.pallas_call(
        functools.partial(pack_kernel, size),
        in_specs=[SMEM, VMEM, VMEM],
        out_specs=[VMEM] * count,
        out_shape=[out] * count,
        compiler_params=ROOM,
        name="pack",
    )(me, mine, other)


def split(x):
    high = x.astype(jnp.bfloat16)
    return high, (x - high.astype(jnp.float32)).astype(jnp.bfloat16)


def collect_kernel(size, part_tiles, *refs):
    messages, (out_ref, *rows_s) = refs[: len(refs) // 2], refs[len(refs) // 2 :]
    pixels = out_ref.shape[1]
    lists = -(-2 * size // LANES)
    flag = jnp.zeros((HEAD, pixels), jnp.float32)
    ids = []
    for message, rows in zip(messages, rows_s):
        rows[...] = jnp.concatenate(split(message[...]), axis=1)
        head = message[size - HEAD : size, :] + message[2 * size - HEAD : 2 * size, :]
        flag = flag + head[lists : lists + 1]
        names = jnp.concatenate([head[i : i + 1] for i in range(lists)], axis=1)[:, : 2 * size]
        ids.append(names.astype(jnp.int32) - 1)
    chunk = min(256, part_tiles)
    for t in range(0, part_tiles, chunk):
        sums = jnp.zeros((chunk, 2 * pixels), jnp.float32)
        for names, rows in zip(ids, rows_s):
            sums = sums + dot(ones_where(iota((chunk, 2 * size), 0) + t == names), rows[...])
        out_ref[t : t + chunk, :] = sums[:, :pixels] + sums[:, pixels:]
    out_ref[part_tiles:, :] = flag


def collect(messages, part_tiles):
    rows, pixels = messages[0].shape
    return pl.pallas_call(
        functools.partial(collect_kernel, rows // 2, part_tiles),
        in_specs=[VMEM] * len(messages),
        out_specs=VMEM,
        out_shape=jax.ShapeDtypeStruct((part_tiles + HEAD, pixels), jnp.float32),
        scratch_shapes=[pltpu.VMEM((rows, 2 * pixels), jnp.bfloat16)] * len(messages),
        compiler_params=ROOM,
        name="collect",
    )(*messages)


def owner_kernel(parts, me_ref, owner_ref, row_ref):
    most = row_ref.shape[1]
    owners = owner_ref[...]
    rows = owners.shape[0]
    mine = owners == me_ref[1] * 2 + me_ref[2]
    marks = jnp.where(mine, 1.0, 0.0)
    rank = running_counts(marks.astype(jnp.bfloat16), rows).astype(jnp.int32) - 1
    index = iota((rows, LANES), 0) * LANES + iota((rows, LANES), 1)
    found = jnp.zeros((HEAD, most), jnp.float32)
    line = iota((HEAD, LANES), 0)
    high, low = bytes_of(index + 1)
    for r in range(rows):
        pieces = jnp.where(line == 0, high[r : r + 1], jnp.where(line == 1, low[r : r + 1], 0.0))
        pieces = jnp.where(mine[r : r + 1], pieces, 0.0)
        spots = ones_where(iota((most, LANES), 0) == rank[r : r + 1])
        found = found + nt_dot(pieces.astype(jnp.bfloat16), spots)
    tile = (found[0:1] * 256.0 + found[1:2]).astype(jnp.int32) - 1
    tile = jnp.where(tile < 0, rows * LANES, tile)
    bounds = jnp.zeros((1, most), jnp.float32)
    for p in range(1, parts + 1):
        before = jnp.where(index < p * (rows * LANES // parts), marks, 0.0)
        bounds = jnp.where(iota((1, most), 1) == p, jnp.sum(before, axis=(0, 1), keepdims=True), bounds)
    row_ref[...] = jnp.where(iota((HEAD, most), 0) == 0, tile, bounds.astype(jnp.int32))


def owned_rows(me, owners, most, parts):
    return pl.pallas_call(
        functools.partial(owner_kernel, parts),
        in_specs=[SMEM, VMEM],
        out_specs=VMEM,
        out_shape=jax.ShapeDtypeStruct((HEAD, most), jnp.int32),
        compiler_params=ROOM,
        name="owned_rows",
    )(me, owners)


def fill_rows(row_ref, moves, start, end, shift):
    unroll = 8

    def one(r):
        at = pl.ds(row_ref[r] - shift, 1)
        for table, rows in moves:
            rows[pl.ds(r, 1), :] = table[at, :]

    def group(i, carry):
        for u in range(unroll):
            one(start + i * unroll + u)
        return carry

    def rest(r, carry):
        one(r)
        return carry

    groups = (end - start) // unroll
    lax.fori_loop(0, groups, group, 0)
    lax.fori_loop(start + groups * unroll, end, rest, 0)


def fill_part(m, me_ref, row_ref, moves):
    most = moves[0][1].shape[0]
    tiles = moves[0][0].shape[0] - HEAD
    part = me_ref[1] ^ m
    fill_rows(row_ref, moves, row_ref[most + part], row_ref[most + part + 1], part * tiles)


def early_kernel(me_ref, row_ref, own_ref, other_ref, own_rows, other_rows, flag_ref):
    tiles = own_ref.shape[0] - HEAD
    flag_ref[0] = jnp.max(own_ref[tiles:, :]).astype(jnp.int32)
    own_rows[...] = jnp.zeros_like(own_rows)
    other_rows[...] = jnp.zeros_like(other_rows)
    fill_part(0, me_ref, row_ref, ((own_ref, own_rows), (other_ref, other_rows)))


def early(me, rows, own, other, most):
    pixels = own.shape[1]
    out = jax.ShapeDtypeStruct((most, pixels), jnp.float32)
    return pl.pallas_call(
        early_kernel,
        in_specs=[SMEM, SMEM, VMEM, VMEM],
        out_specs=[VMEM, VMEM, SMEM],
        out_shape=[out, out, jax.ShapeDtypeStruct((1,), jnp.int32)],
        compiler_params=ROOM,
        name="early",
    )(me, rows, own, other)


def middle_kernel(me_ref, row_ref, before_ref, *refs):
    pieces, rows_ref = refs[:-1], refs[-1]
    rows_ref[...] = before_ref[...]
    for m, piece in enumerate(pieces, 1):
        fill_part(m, me_ref, row_ref, ((piece, rows_ref),))


def middle(me, rows, before, pieces):
    return pl.pallas_call(
        middle_kernel,
        in_specs=[SMEM, SMEM, VMEM] + [VMEM] * len(pieces),
        out_specs=VMEM,
        out_shape=jax.ShapeDtypeStruct(before.shape, jnp.float32),
        compiler_params=ROOM,
        name="middle",
    )(me, rows, before, *pieces)


def late_kernel(me_ref, row_ref, own_rows, before_ref, *refs):
    pieces, (owned_ref, map_ref, other_rows) = refs[:-3], refs[-3:]
    tiles, pixels = pieces[0].shape[0] - HEAD, pieces[0].shape[1]
    lower = me_ref[2] == 0

    def put(ref, at, own, other):
        ref[at, :pixels] = jnp.where(lower, own, other)
        ref[at, pixels:] = jnp.where(lower, other, own)

    other_rows[...] = before_ref[...]
    for m in range(len(pieces) // 2):
        own, other = pieces[2 * m], pieces[2 * m + 1]
        at = pl.ds(pl.multiple_of((me_ref[1] ^ m) * tiles, tiles), tiles)
        put(map_ref, at, own[:tiles, :], other[:tiles, :])
        if m:
            fill_part(m, me_ref, row_ref, ((other, other_rows),))
    put(owned_ref, slice(None), own_rows[...], other_rows[...])


def late(me, rows, own_rows, before, pieces, block):
    most, pixels = own_rows.shape
    return pl.pallas_call(
        late_kernel,
        in_specs=[SMEM, SMEM] + [VMEM] * (2 + len(pieces)),
        out_specs=[VMEM, VMEM],
        out_shape=[
            jax.ShapeDtypeStruct((most, 2 * pixels), jnp.float32),
            jax.ShapeDtypeStruct((block, 2 * pixels), jnp.float32),
        ],
        scratch_shapes=[pltpu.VMEM((most, pixels), jnp.float32)],
        compiler_params=ROOM,
        name="late",
    )(me, rows, own_rows, before, *pieces)


def shards(kernel, pressure, velocity, entry_slot, slot_tile, tile_owner):
    vols = lax.axis_size("vol")
    pixs = lax.axis_size("pix")
    vol = lax.axis_index("vol")
    pix = lax.axis_index("pix")
    entries, _ = kernel.shape
    slots = slot_tile.shape[1]
    block = tile_owner.shape[0] // vols
    parts = pixs // 2
    part_tiles = block // parts
    half = vols // 2
    most_owned = 2 * block // pixs
    most_rows = min(2 * slots // vols, part_tiles)
    me = jnp.stack([vol, pix >> 1, pix & 1]).astype(jnp.int32)
    tiles = slot_tile.reshape(slots // LANES, LANES)
    slot = entry_slot.reshape(entries // LANES, LANES)
    factors = [x.reshape(entries // LANES, LANES) for x in (pressure, velocity)]
    owners = lax.dynamic_slice_in_dim(
        tile_owner.reshape(vols, block // LANES, LANES), vol, 1
    )[0]
    rows = owned_rows(me, owners, most_owned, parts)[:2].reshape(-1)

    def send(x, vol_step=0, part_step=0, core_step=0):
        step = (vol_step * parts + part_step) * 2 + core_step
        return lax.ppermute(x, ("vol", "pix"), [(d, d ^ step) for d in range(vols * pixs)])

    def exchange(cap):
        size = cap + HEAD
        place, ends, head = plan(me, tiles, slot, vols, parts, block, cap)
        far, near, far_other, near_other = project(
            me, kernel, factors, slot, ends.reshape(-1), place.reshape(-1), head, cap
        )

        def gather(own, other):
            taken = send(other, core_step=1)
            messages = list(pack(me, own, taken, size))
            for k in reversed(range(1, len(messages))):
                messages[k] = send(messages[k], k // parts, k % parts)
            return collect(messages, part_tiles)

        crossed = send(gather(far, far_other), vol_step=half)
        mine = gather(near, near_other) + crossed
        other = send(mine, core_step=1)
        own_rows, other_rows, flag = early(me, rows, mine, other, most_owned)
        across = [send(mine, part_step=m) for m in range(1, parts)]
        pieces = [mine, other]
        for piece in across:
            pieces += [piece, send(piece, core_step=1)]
        own_rows = middle(me, rows, own_rows, across)
        return flag[0] > 0, *late(me, rows, own_rows, other_rows, pieces, block)

    result = exchange(most_rows * 13 // 32 // 8 * 8)

    def redo(state):
        unused, *full = exchange(most_rows)
        return jnp.zeros((), bool), *full

    _, owned, shell = lax.while_loop(lambda state: state[0], redo, result)
    return owned, shell


def solution(mesh):
    in_specs = (
        P(("vol", "pix"), None),
        P(("vol", "pix")),
        P(("vol", "pix")),
        P(("vol", "pix"), None),
        P(("vol", "pix"), None),
        P(),
    )
    out_specs = (P(("vol", "pix"), None), P("vol", None))
    return jax.shard_map(shards, mesh=mesh, in_specs=in_specs, out_specs=out_specs, check_vma=False)
```

```python
import functools

import jax
import jax.numpy as jnp
from jax import lax
from jax.experimental import pallas as pl
from jax.experimental.pallas import tpu as pltpu
from jax.sharding import PartitionSpec as P


LANES = 128
HEAD = 8
ROOM = pltpu.CompilerParams(vmem_limit_bytes=16 << 20)
GROUP = 256
WINDOW = 40
SUBS = 2


SMEM = pl.BlockSpec(memory_space=pltpu.SMEM)
VMEM = pl.BlockSpec(memory_space=pltpu.VMEM)
ANY = pl.BlockSpec(memory_space=pl.ANY)
HBM = pl.BlockSpec(memory_space=pltpu.HBM)


def iota(shape, axis):
    return lax.broadcasted_iota(jnp.int32, shape, axis)


def nt_dot(a, b):
    return lax.dot_general(a, b, (((1,), (1,)), ((), ())), preferred_element_type=jnp.float32)


def dot(a, b):
    return jnp.dot(a, b, preferred_element_type=jnp.float32)


def ones_where(mask):
    return jnp.where(mask, 1.0, 0.0).astype(jnp.bfloat16)


def bytes_of(x):
    return (x >> 8).astype(jnp.float32), (x & 255).astype(jnp.float32)


def running_counts(marks, rows):
    total = marks.shape[0]
    upper = ones_where(iota((LANES, LANES), 0) <= iota((LANES, LANES), 1))
    row, column = iota((total, total), 0), iota((total, total), 1)
    earlier = ones_where((column < row) & (row // rows == column // rows))
    before = dot(earlier, marks).astype(jnp.bfloat16)
    return dot(marks, upper) + dot(before, jnp.ones((LANES, LANES), jnp.bfloat16))


def line_ends(slots):
    lane, line = iota((HEAD, LANES), 1), iota((HEAD, LANES), 0)
    ends = ones_where(((line == 0) & (lane == 0)) | ((line == 1) & (lane == LANES - 1)))
    high, low = bytes_of(slots)
    ends = nt_dot(ends, high.astype(jnp.bfloat16)) * 256.0 + nt_dot(ends, low.astype(jnp.bfloat16))
    return ends.astype(jnp.int32)


def order_slots(tiles, group, classes, cap, core):
    rows = tiles.shape[0]
    marks = jnp.concatenate([jnp.where(group == i, 1.0, 0.0) for i in range(classes)], axis=0)
    counts = running_counts(marks.astype(jnp.bfloat16), rows) * marks
    place = jnp.zeros((rows, LANES), jnp.float32)
    for i in range(classes):
        place = place + counts[i * rows : (i + 1) * rows]
    place = place.astype(jnp.int32) - 1
    fits = place < cap
    return jnp.where(core == 0, place, cap - 1 - place), fits, counts


def message_heads(tiles, group, place, fits, counts, classes, cap, both, core):
    rows = tiles.shape[0]
    line = iota((HEAD, LANES), 0)
    spilled = jnp.sum(jnp.where(fits, 0.0, 1.0), axis=(0, 1), keepdims=True)
    lists = -(-both // LANES)
    width = lists * LANES
    spot = jnp.where(fits, place + core * (both - cap), -1)
    high, low = bytes_of(tiles + 1)
    ids = jnp.zeros((2 * classes, width), jnp.float32)
    which = iota((classes, LANES), 0)
    for r in range(rows):
        here = group[r : r + 1] == which
        pieces = jnp.concatenate(
            [jnp.where(here, high[r : r + 1], 0.0), jnp.where(here, low[r : r + 1], 0.0)], axis=0
        )
        spots = ones_where(iota((width, LANES), 0) == spot[r : r + 1])
        ids = ids + nt_dot(pieces.astype(jnp.bfloat16), spots)
    ids = ids[:classes] * 256.0 + ids[classes:]
    heads = []
    for k in range(classes):
        held = jnp.max(counts[k * rows : (k + 1) * rows], axis=(0, 1), keepdims=True)
        head = jnp.where(line == lists, jnp.broadcast_to(spilled, (HEAD, LANES)), 0.0)
        head = jnp.where(line == lists + 1, jnp.broadcast_to(held, (HEAD, LANES)), head)
        for i in range(lists):
            head = jnp.where(line == i, ids[k : k + 1, i * LANES : (i + 1) * LANES], head)
        heads.append(head)
    return heads


def project_kernel(
    steps, vols, parts, block, cap, both, me_ref, tile_ref, kernel_hbm, thermal_ref, kinetic_ref, slot_ref,
    own_out, other_out, kernel_ref, own_ref, other_ref, own_s, other_s,
    place_v, ends_v, place_ref, ends_ref, in_sem, table_sem
):
    entries, _ = kernel_ref.shape
    part = entries // steps
    groups = part // GROUP
    lines = GROUP // LANES
    size = cap + HEAD
    classes = vols * parts
    core = me_ref[2]

    def load(step):
        piece = pl.ds(pl.multiple_of(step * part, part), part)
        return pltpu.make_async_copy(kernel_hbm.at[piece], kernel_ref.at[piece], in_sem.at[step])

    for step in range(steps):
        load(step).start()
    ends_v[...] = line_ends(slot_ref[...])
    tiles = tile_ref[...]
    piece = tiles // (block // parts)
    tiles = tiles - piece * (block // parts)
    group_of = piece ^ (me_ref[0] * parts + me_ref[1])
    place, fits, counts = order_slots(tiles, group_of, classes, cap, core)
    place_v[...] = jnp.where(fits, group_of * size + place, classes * size - 1)
    for ref in (own_ref, other_ref, own_out, other_out):
        ref[...] = jnp.zeros_like(ref)
    thermal, kinetic = thermal_ref[...].astype(jnp.float32), kinetic_ref[...].astype(jnp.float32)
    own_s[...] = jnp.where(core == 0, thermal, kinetic)
    other_s[...] = jnp.where(core == 0, kinetic, thermal)
    tables = [
        pltpu.make_async_copy(ends_v, ends_ref, table_sem.at[0]),
        pltpu.make_async_copy(place_v, place_ref, table_sem.at[1]),
    ]
    for table in tables:
        table.start()
    heads = message_heads(tiles, group_of, place, fits, counts, classes, cap, both, core)
    for table in tables:
        table.wait()
    line = iota((WINDOW, LANES), 0)

    def first(group):
        return ends_ref[0, group * lines] & -8

    def reach(group):
        return ends_ref[1, group * lines + lines - 1] - first(group)

    def add(group, base):
        own, other = [], []
        for r in range(lines):
            at = pl.ds(group * lines + r, 1)
            match = line == slot_ref[at, :] - base
            own.append(jnp.where(match, own_s[at, :], 0.0))
            other.append(jnp.where(match, other_s[at, :], 0.0))
        weights = jnp.concatenate(
            [jnp.concatenate(own, axis=1), jnp.concatenate(other, axis=1)], axis=0
        ).astype(jnp.bfloat16)
        sums = dot(weights, kernel_ref[pl.ds(pl.multiple_of(group * GROUP, GROUP), GROUP), :])
        window = pl.ds(pl.multiple_of(base, 8), WINDOW)
        own_ref[window, :] += sums[:WINDOW]
        other_ref[window, :] += sums[WINDOW:]

    def turn(step, most):
        load(step).wait()
        for g in range(groups):
            group = step * groups + g
            add(group, first(group))
            most = jnp.maximum(most, reach(group))
        return most

    most = lax.fori_loop(0, steps, turn, 0)

    @pl.when(most >= WINDOW)
    def _():
        def more(group, carry):
            def again(w, inner):
                add(group, first(group) + w * WINDOW)
                return inner

            return lax.fori_loop(1, reach(group) // WINDOW + 1, again, carry)

        lax.fori_loop(0, steps * groups, more, 0)

    unroll = 16
    turns = LANES // unroll

    def move(i, carry):
        row, lane = i // turns, i % turns * unroll
        for u in range(unroll):
            to, at = pl.ds(place_ref[row, lane + u], 1), pl.ds(i * unroll + u, 1)
            own_out[to, :] = own_ref[at, :]
            other_out[to, :] = other_ref[at, :]
        return carry

    lax.fori_loop(0, place_ref.shape[0] * turns, move, 0)
    for out in (own_out, other_out):
        for k, head in enumerate(heads):
            out[k * size + cap : (k + 1) * size, :] = head


def project(me, kernel, factors, slot, tiles, vols, parts, block, cap, both):
    entries, pixels = kernel.shape
    steps = 4
    rows = vols * parts * (cap + HEAD)
    partial = pltpu.VMEM((tiles.shape[0] * LANES + WINDOW, pixels), jnp.float32)
    factor = pltpu.VMEM(slot.shape, jnp.float32)
    ends = (HEAD, slot.shape[0])
    return pl.pallas_call(
        functools.partial(project_kernel, steps, vols, parts, block, cap, both),
        in_specs=[SMEM, VMEM, HBM, VMEM, VMEM, VMEM],
        out_specs=[VMEM] * 2,
        out_shape=[jax.ShapeDtypeStruct((rows, pixels), jnp.float32)] * 2,
        scratch_shapes=[
            pltpu.VMEM((entries, pixels), kernel.dtype),
            partial, partial, factor, factor,
            pltpu.VMEM(tiles.shape, jnp.int32), pltpu.VMEM(ends, jnp.int32),
            pltpu.SMEM(tiles.shape, jnp.int32), pltpu.SMEM(ends, jnp.int32),
            pltpu.SemaphoreType.DMA((steps,)), pltpu.SemaphoreType.DMA((2,)),
        ],
        compiler_params=ROOM,
        name="project",
    )(me, tiles, kernel, *factors, slot)


def pack_kernel(cap, both, me_ref, mine_ref, other_ref, *outs):
    size = cap + HEAD
    lists = -(-both // LANES)
    lower = me_ref[2] == 0
    line = iota((HEAD, LANES), 0)
    heads, spilled = [], jnp.zeros((1, LANES), jnp.float32)
    for k, out in enumerate(outs):
        mine, other = mine_ref[k * size : (k + 1) * size, :], other_ref[k * size : (k + 1) * size, :]
        one, two = jnp.where(lower, mine, other), jnp.where(lower, other, mine)
        out[:cap, :] = one[:cap]
        if both > 2 * cap:
            out[cap : both - cap, :] = jnp.zeros((both - 2 * cap, LANES), jnp.float32)
        shared = max(2 * cap - both, 0)
        if shared:
            out[cap - shared : cap, :] = one[cap - shared : cap] + two[:shared]
        out[cap + max(both - 2 * cap, 0) : both, :] = two[shared:cap]
        head = one[cap:] + two[cap:]
        heads.append(head)
        spilled = spilled + head[lists : lists + 1] + jnp.maximum(head[lists + 1 : lists + 2] - both, 0.0)
    for out, head in zip(outs, heads):
        out[both:, :] = jnp.where(line == lists, spilled, head)


def pack(me, mine, other, cap, both):
    count = mine.shape[0] // (cap + HEAD)
    out = jax.ShapeDtypeStruct((both + HEAD, mine.shape[1]), jnp.float32)
    return pl.pallas_call(
        functools.partial(pack_kernel, cap, both),
        in_specs=[SMEM, VMEM, VMEM],
        out_specs=[VMEM] * count,
        out_shape=[out] * count,
        compiler_params=ROOM,
        name="pack",
    )(me, mine, other)


def split(x):
    high = x.astype(jnp.bfloat16)
    return high, (x - high.astype(jnp.float32)).astype(jnp.bfloat16)


def collect_kernel(count, sub_tiles, *refs):
    messages, outs, rows_s = refs[:count], refs[count : count + SUBS], refs[count + SUBS :]
    both, pixels = messages[0].shape[0] - HEAD, messages[0].shape[1]
    lists = -(-both // LANES)
    flag = jnp.zeros((HEAD, pixels), jnp.float32)
    ids = []
    for message, rows in zip(messages, rows_s):
        rows[...] = jnp.concatenate(split(message[:both, :]), axis=1)
        head = message[both:, :]
        flag = flag + head[lists : lists + 1]
        names = jnp.concatenate([head[i : i + 1] for i in range(lists)], axis=1)[:, :both]
        ids.append(names.astype(jnp.int32) - 1)
    chunk = min(256, sub_tiles)
    for sub, out_ref in enumerate(outs):
        for t in range(0, sub_tiles, chunk):
            sums = jnp.zeros((chunk, 2 * pixels), jnp.float32)
            for names, rows in zip(ids, rows_s):
                hit = ones_where(iota((chunk, both), 0) + (sub * sub_tiles + t) == names)
                sums = sums + dot(hit, rows[...])
            out_ref[t : t + chunk, :] = sums[:, :pixels] + sums[:, pixels:]
        out_ref[sub_tiles:, :] = flag


def collect(messages, sub_tiles):
    rows, pixels = messages[0].shape
    return pl.pallas_call(
        functools.partial(collect_kernel, len(messages), sub_tiles),
        in_specs=[VMEM] * len(messages),
        out_specs=[VMEM] * SUBS,
        out_shape=[jax.ShapeDtypeStruct((sub_tiles + HEAD, pixels), jnp.float32)] * SUBS,
        scratch_shapes=[pltpu.VMEM((rows - HEAD, 2 * pixels), jnp.bfloat16)] * len(messages),
        compiler_params=ROOM,
        name="collect",
    )(*messages)


def owner_kernel(parts, me_ref, owner_ref, row_ref):
    most = row_ref.shape[1]
    owners = owner_ref[...]
    rows = owners.shape[0]
    mine = owners == me_ref[1] * 2 + me_ref[2]
    marks = jnp.where(mine, 1.0, 0.0)
    rank = running_counts(marks.astype(jnp.bfloat16), rows).astype(jnp.int32) - 1
    index = iota((rows, LANES), 0) * LANES + iota((rows, LANES), 1)
    found = jnp.zeros((HEAD, most), jnp.float32)
    line = iota((HEAD, LANES), 0)
    high, low = bytes_of(index + 1)
    for r in range(rows):
        pieces = jnp.where(line == 0, high[r : r + 1], jnp.where(line == 1, low[r : r + 1], 0.0))
        pieces = jnp.where(mine[r : r + 1], pieces, 0.0)
        spots = ones_where(iota((most, LANES), 0) == rank[r : r + 1])
        found = found + nt_dot(pieces.astype(jnp.bfloat16), spots)
    tile = (found[0:1] * 256.0 + found[1:2]).astype(jnp.int32) - 1
    tile = jnp.where(tile < 0, rows * LANES, tile)
    bounds = jnp.zeros((1, most), jnp.float32)
    for p in range(1, SUBS * parts + 1):
        before = jnp.where(index < p * (rows * LANES // (SUBS * parts)), marks, 0.0)
        bounds = jnp.where(iota((1, most), 1) == p, jnp.sum(before, axis=(0, 1), keepdims=True), bounds)
    row_ref[...] = jnp.where(iota((HEAD, most), 0) == 0, tile, bounds.astype(jnp.int32))


def owned_rows(me, owners, most, parts):
    return pl.pallas_call(
        functools.partial(owner_kernel, parts),
        in_specs=[SMEM, VMEM],
        out_specs=VMEM,
        out_shape=jax.ShapeDtypeStruct((HEAD, most), jnp.int32),
        compiler_params=ROOM,
        name="owned_rows",
    )(me, owners)


def fill_rows(row_ref, moves, start, end, shift):
    unroll = 8

    def one(r):
        at = pl.ds(row_ref[r] - shift, 1)
        for table, rows in moves:
            rows[pl.ds(r, 1), :] = table[at, :]

    def group(i, carry):
        for u in range(unroll):
            one(start + i * unroll + u)
        return carry

    def rest(r, carry):
        one(r)
        return carry

    groups = (end - start) // unroll
    lax.fori_loop(0, groups, group, 0)
    lax.fori_loop(start + groups * unroll, end, rest, 0)


def fill_part(m, sub, me_ref, row_ref, moves):
    most = moves[0][1].shape[0]
    tiles = moves[0][0].shape[0] - HEAD
    at = (me_ref[1] ^ m) * SUBS + sub
    fill_rows(row_ref, moves, row_ref[most + at], row_ref[most + at + 1], at * tiles)


def early_kernel(me_ref, row_ref, *refs):
    pieces, (own_rows, other_rows, flag_ref) = refs[:-3], refs[-3:]
    own, other = pieces[:SUBS], pieces[SUBS:]
    tiles = own[0].shape[0] - HEAD
    flag_ref[0] = jnp.max(own[0][tiles:, :]).astype(jnp.int32)
    own_rows[...] = jnp.zeros_like(own_rows)
    other_rows[...] = jnp.zeros_like(other_rows)
    for sub in range(SUBS):
        fill_part(0, sub, me_ref, row_ref, ((own[sub], own_rows), (other[sub], other_rows)))


def early(me, rows, own, other, most):
    out = jax.ShapeDtypeStruct((most, own[0].shape[1]), jnp.float32)
    return pl.pallas_call(
        early_kernel,
        in_specs=[SMEM, SMEM] + [VMEM] * (2 * SUBS),
        out_specs=[VMEM, VMEM, SMEM],
        out_shape=[out, out, jax.ShapeDtypeStruct((1,), jnp.int32)],
        compiler_params=ROOM,
        name="early",
    )(me, rows, *own, *other)


def middle_kernel(me_ref, row_ref, before_ref, *refs):
    pieces, rows_ref = refs[:-1], refs[-1]
    rows_ref[...] = before_ref[...]
    for i, piece in enumerate(pieces):
        fill_part(1 + i // SUBS, i % SUBS, me_ref, row_ref, ((piece, rows_ref),))


def middle(me, rows, before, pieces):
    return pl.pallas_call(
        middle_kernel,
        in_specs=[SMEM, SMEM, VMEM] + [VMEM] * len(pieces),
        out_specs=VMEM,
        out_shape=jax.ShapeDtypeStruct(before.shape, jnp.float32),
        compiler_params=ROOM,
        name="middle",
    )(me, rows, before, *pieces)


def late_kernel(me_ref, row_ref, own_rows, before_ref, *refs):
    pieces, (owned_ref, map_ref, other_rows) = refs[:-3], refs[-3:]
    tiles, pixels = pieces[0].shape[0] - HEAD, pieces[0].shape[1]
    half = len(pieces) // 2
    lower = me_ref[2] == 0

    def put(ref, at, own, other):
        ref[at, :pixels] = jnp.where(lower, own, other)
        ref[at, pixels:] = jnp.where(lower, other, own)

    other_rows[...] = before_ref[...]
    for i in range(half):
        own, other = pieces[i], pieces[half + i]
        m, sub = i // SUBS, i % SUBS
        at = pl.multiple_of(((me_ref[1] ^ m) * SUBS + sub) * tiles, tiles)
        put(map_ref, pl.ds(at, tiles), own[:tiles, :], other[:tiles, :])
        if m:
            fill_part(m, sub, me_ref, row_ref, ((other, other_rows),))
    put(owned_ref, slice(None), own_rows[...], other_rows[...])


def late(me, rows, own_rows, before, own, other, block):
    most, pixels = own_rows.shape
    return pl.pallas_call(
        late_kernel,
        in_specs=[SMEM, SMEM] + [VMEM] * (2 + len(own) + len(other)),
        out_specs=[VMEM, VMEM],
        out_shape=[
            jax.ShapeDtypeStruct((most, 2 * pixels), jnp.float32),
            jax.ShapeDtypeStruct((block, 2 * pixels), jnp.float32),
        ],
        scratch_shapes=[pltpu.VMEM((most, pixels), jnp.float32)],
        compiler_params=ROOM,
        name="late",
    )(me, rows, own_rows, before, *own, *other)


def shards(kernel, pressure, velocity, entry_slot, slot_tile, tile_owner):
    vols = lax.axis_size("vol")
    pixs = lax.axis_size("pix")
    vol = lax.axis_index("vol")
    pix = lax.axis_index("pix")
    entries, _ = kernel.shape
    slots = slot_tile.shape[1]
    block = tile_owner.shape[0] // vols
    parts = pixs // 2
    part_tiles = block // parts
    half = vols // 2
    most_owned = 2 * block // pixs
    most_rows = min(2 * slots // vols, part_tiles)
    me = jnp.stack([vol, pix >> 1, pix & 1]).astype(jnp.int32)
    tiles = slot_tile.reshape(slots // LANES, LANES)
    slot = entry_slot.reshape(entries // LANES, LANES)
    factors = [x.reshape(entries // LANES, LANES) for x in (pressure, velocity)]
    owners = lax.dynamic_slice_in_dim(
        tile_owner.reshape(vols, block // LANES, LANES), vol, 1
    )[0]
    rows = owned_rows(me, owners, most_owned, parts)[:2].reshape(-1)

    def send(x, vol_step=0, part_step=0, core_step=0):
        step = (vol_step * parts + part_step) * 2 + core_step
        return lax.ppermute(x, ("vol", "pix"), [(d, d ^ step) for d in range(vols * pixs)])

    def exchange(cap, both):
        count = half * parts
        own, given = project(me, kernel, factors, slot, tiles, vols, parts, block, cap, both)
        messages = pack(me, own, send(given, core_step=1), cap, both)

        def gather(messages):
            messages = list(messages)
            for k in reversed(range(1, count)):
                messages[k] = send(messages[k], k // parts, k % parts)
            return collect(messages, part_tiles // SUBS)

        far = gather(messages[count:])
        crossed = [send(x, vol_step=half) for x in far]
        near = gather(messages[:count])
        mine = [x + y for x, y in zip(near, crossed)]
        other = [send(x, core_step=1) for x in mine]
        own_rows, other_rows, flag = early(me, rows, mine, other, most_owned)
        across = [send(x, part_step=m) for m in range(1, parts) for x in mine]
        beyond = [send(x, core_step=1) for x in across]
        own_rows = middle(me, rows, own_rows, across)
        full = late(me, rows, own_rows, other_rows, mine + across, other + beyond, block)
        return flag[0] > 0, *full

    def rows_of(share):
        return most_rows * share // 32 // 8 * 8

    result = exchange(rows_of(13), rows_of(24))

    def redo(state):
        unused, *full = exchange(most_rows, 2 * most_rows)
        return jnp.zeros((), bool), *full

    _, owned, shell = lax.while_loop(lambda state: state[0], redo, result)
    return owned, shell


def solution(mesh):
    in_specs = (
        P(("vol", "pix"), None),
        P(("vol", "pix")),
        P(("vol", "pix")),
        P(("vol", "pix"), None),
        P(("vol", "pix"), None),
        P(),
    )
    out_specs = (P(("vol", "pix"), None), P("vol", None))
    return jax.shard_map(shards, mesh=mesh, in_specs=in_specs, out_specs=out_specs, check_vma=False)
```

```python
import functools

import jax
import jax.numpy as jnp
from jax import lax
from jax.experimental import pallas as pl
from jax.experimental.pallas import tpu as pltpu
from jax.sharding import PartitionSpec as P


LANES = 128
HEAD = 8
ROOM = pltpu.CompilerParams(vmem_limit_bytes=16 << 20)
GROUP = 256
WINDOW = 40
SUBS = 2


SMEM = pl.BlockSpec(memory_space=pltpu.SMEM)
VMEM = pl.BlockSpec(memory_space=pltpu.VMEM)
ANY = pl.BlockSpec(memory_space=pl.ANY)
HBM = pl.BlockSpec(memory_space=pltpu.HBM)


def iota(shape, axis):
    return lax.broadcasted_iota(jnp.int32, shape, axis)


def nt_dot(a, b):
    return lax.dot_general(a, b, (((1,), (1,)), ((), ())), preferred_element_type=jnp.float32)


def dot(a, b):
    return jnp.dot(a, b, preferred_element_type=jnp.float32)


def ones_where(mask):
    return jnp.where(mask, 1.0, 0.0).astype(jnp.bfloat16)


def bytes_of(x):
    return (x >> 8).astype(jnp.float32), (x & 255).astype(jnp.float32)


def running_counts(marks, rows):
    total = marks.shape[0]
    upper = ones_where(iota((LANES, LANES), 0) <= iota((LANES, LANES), 1))
    row, column = iota((total, total), 0), iota((total, total), 1)
    earlier = ones_where((column < row) & (row // rows == column // rows))
    before = dot(earlier, marks).astype(jnp.bfloat16)
    return dot(marks, upper) + dot(before, jnp.ones((LANES, LANES), jnp.bfloat16))


def class_order(count):
    return sorted(range(count), key=lambda k: (bin(k).count("1") % 2, k))


def plan_kernel(vols, parts, block, cap, both, me_ref, tile_ref, slot_ref, place_ref, ends_ref, head_ref):
    size = cap + HEAD
    part_tiles = block // parts
    lane = iota((HEAD, LANES), 1)
    line = iota((HEAD, LANES), 0)
    slots = slot_ref[...]
    ends = ones_where(((line == 0) & (lane == 0)) | ((line == 1) & (lane == LANES - 1)))
    high, low = bytes_of(slots)
    ends_ref[...] = (
        nt_dot(ends, high.astype(jnp.bfloat16)) * 256.0 + nt_dot(ends, low.astype(jnp.bfloat16))
    ).astype(jnp.int32)

    tiles = tile_ref[...]
    rows = tiles.shape[0]
    classes = vols * parts
    part = tiles // part_tiles
    group = part ^ (me_ref[0] * parts + me_ref[1])
    marks = jnp.concatenate([jnp.where(group == i, 1.0, 0.0) for i in range(classes)], axis=0)
    counts = running_counts(marks.astype(jnp.bfloat16), rows) * marks
    place = jnp.zeros((rows, LANES), jnp.float32)
    for i in range(classes):
        place = place + counts[i * rows : (i + 1) * rows]
    place = place.astype(jnp.int32) - 1
    fits = place < cap
    spilled = jnp.sum(jnp.where(fits, 0.0, 1.0), axis=(0, 1), keepdims=True)
    count = classes // 2
    quarter = count // 2
    box = jnp.zeros_like(group)
    held = jnp.zeros((1, LANES), jnp.float32)
    for far in range(2):
        for i, k in enumerate(class_order(count)):
            server, j = divmod(i, quarter)
            name = far * count + k
            here = jnp.where(me_ref[2] == server, 0, count) + (far * quarter + j)
            box = jnp.where(group == name, here, box)
            most = jnp.max(counts[name * rows : (name + 1) * rows], axis=(0, 1), keepdims=True)
            held = jnp.where(iota((1, LANES), 1) == name, most, held)
    place = jnp.where(me_ref[2] == 0, place, cap - 1 - place)
    place_ref[...] = jnp.where(fits, box * size + place, classes * size)
    lists = -(-both // LANES)
    width = lists * LANES
    spot = jnp.where(fits, place + me_ref[2] * (both - cap), -1)
    high, low = bytes_of(tiles - part * part_tiles + 1)
    ids = jnp.zeros((2 * classes, width), jnp.float32)
    which = iota((classes, LANES), 0)
    for r in range(rows):
        here = box[r : r + 1] == which
        pieces = jnp.concatenate(
            [jnp.where(here, high[r : r + 1], 0.0), jnp.where(here, low[r : r + 1], 0.0)], axis=0
        )
        spots = ones_where(iota((width, LANES), 0) == spot[r : r + 1])
        ids = ids + nt_dot(pieces.astype(jnp.bfloat16), spots)
    ids = ids[:classes] * 256.0 + ids[classes:]
    for k in range(classes):
        head = jnp.where(line == lists, jnp.broadcast_to(spilled, (HEAD, LANES)), 0.0)
        head = jnp.where(line == lists + 1, held, head)
        for i in range(lists):
            head = jnp.where(line == i, ids[k : k + 1, i * LANES : (i + 1) * LANES], head)
        head_ref[k * HEAD : (k + 1) * HEAD, :] = head


def plan(me, tiles, slot, vols, parts, block, cap, both):
    rows = tiles.shape[0]
    return pl.pallas_call(
        functools.partial(plan_kernel, vols, parts, block, cap, both),
        in_specs=[SMEM, VMEM, VMEM],
        out_specs=[VMEM, VMEM, VMEM],
        out_shape=[
            jax.ShapeDtypeStruct((rows, LANES), jnp.int32),
            jax.ShapeDtypeStruct((HEAD, slot.shape[0]), jnp.int32),
            jax.ShapeDtypeStruct((vols * parts * HEAD, LANES), jnp.float32),
        ],
        compiler_params=ROOM,
        name="plan",
    )(me, tiles, slot)


def project_kernel(
    steps, cap, me_ref, ends_ref, place_ref, kernel_hbm, thermal_ref, kinetic_ref, slot_ref, head_ref,
    held_thermal, held_kinetic, given_ref,
    kernel_ref, own_ref, other_ref, own_stage, other_stage, own_s, other_s, in_sem
):
    entries, _ = kernel_ref.shape
    part = entries // steps
    groups = part // GROUP
    lines = GROUP // LANES
    slots = place_ref.shape[0]
    total = entries // LANES

    def load(step):
        piece = pl.ds(pl.multiple_of(step * part, part), part)
        return pltpu.make_async_copy(kernel_hbm.at[piece], kernel_ref.at[piece], in_sem.at[step])

    for step in range(steps):
        load(step).start()
    for ref in (own_ref, other_ref, own_stage, other_stage):
        ref[...] = jnp.zeros_like(ref)
    own_s[...] = thermal_ref[...].astype(jnp.float32)
    other_s[...] = kinetic_ref[...].astype(jnp.float32)
    line = iota((WINDOW, LANES), 0)

    def first(group):
        return ends_ref[group * lines] & -8

    def reach(group):
        return ends_ref[total + group * lines + lines - 1] - first(group)

    def add(group, base):
        own, other = [], []
        for r in range(lines):
            at = pl.ds(group * lines + r, 1)
            match = line == slot_ref[at, :] - base
            own.append(jnp.where(match, own_s[at, :], 0.0))
            other.append(jnp.where(match, other_s[at, :], 0.0))
        weights = jnp.concatenate(
            [jnp.concatenate(own, axis=1), jnp.concatenate(other, axis=1)], axis=0
        ).astype(jnp.bfloat16)
        sums = dot(weights, kernel_ref[pl.ds(pl.multiple_of(group * GROUP, GROUP), GROUP), :])
        window = pl.ds(pl.multiple_of(base, 8), WINDOW)
        own_ref[window, :] += sums[:WINDOW]
        other_ref[window, :] += sums[WINDOW:]

    def turn(step, most):
        load(step).wait()
        for g in range(groups):
            group = step * groups + g
            add(group, first(group))
            most = jnp.maximum(most, reach(group))
        return most

    most = lax.fori_loop(0, steps, turn, 0)

    @pl.when(most >= WINDOW)
    def _():
        def more(group, carry):
            def again(w, inner):
                add(group, first(group) + w * WINDOW)
                return inner

            return lax.fori_loop(1, reach(group) // WINDOW + 1, again, carry)

        lax.fori_loop(0, steps * groups, more, 0)

    unroll = 16

    def move(i, carry):
        for u in range(unroll):
            s = i * unroll + u
            to = place_ref[s]
            own_stage[pl.ds(to, 1), :] = own_ref[pl.ds(s, 1), :]
            other_stage[pl.ds(to, 1), :] = other_ref[pl.ds(s, 1), :]
        return carry

    lax.fori_loop(0, slots // unroll, move, 0)
    size = cap + HEAD
    count = head_ref.shape[0] // HEAD // 2
    for channel, (held, stage) in enumerate(((held_thermal, own_stage), (held_kinetic, other_stage))):
        for k in range(2 * count):
            out, at = (held, k * size) if k < count else (given_ref, (channel * count + k - count) * size)
            out[at : at + cap, :] = stage[k * size : k * size + cap, :]
            out[at + cap : at + size, :] = head_ref[k * HEAD : (k + 1) * HEAD, :]


def project(me, kernel, factors, slot, ends, place, head, cap):
    entries, pixels = kernel.shape
    slots = place.shape[0]
    steps = 4
    rows = head.shape[0] // HEAD * (cap + HEAD)
    partial = pltpu.VMEM((slots + WINDOW, pixels), jnp.float32)
    stage = pltpu.VMEM((rows + HEAD, pixels), jnp.float32)
    factor = pltpu.VMEM(slot.shape, jnp.float32)
    half = jax.ShapeDtypeStruct((rows // 2, pixels), jnp.float32)
    return pl.pallas_call(
        functools.partial(project_kernel, steps, cap),
        in_specs=[SMEM, SMEM, SMEM, HBM, VMEM, VMEM, VMEM, VMEM],
        out_specs=[VMEM] * 3,
        out_shape=[half, half, jax.ShapeDtypeStruct((rows, pixels), jnp.float32)],
        scratch_shapes=[
            pltpu.VMEM((entries, pixels), kernel.dtype),
            partial, partial, stage, stage, factor, factor,
            pltpu.SemaphoreType.DMA((steps,)),
        ],
        compiler_params=ROOM,
        name="project",
    )(me, ends, place, kernel, *factors, slot, head)


def pack_kernel(cap, both, me_ref, thermal_ref, kinetic_ref, taken_ref, *outs):
    size, count = cap + HEAD, len(outs)
    lists = -(-both // LANES)
    lower = me_ref[2] == 0
    line = iota((HEAD, LANES), 0)
    shared = max(2 * cap - both, 0)
    spilled = None
    for k, out in enumerate(outs):
        for channel, held in enumerate((thermal_ref, kinetic_ref)):
            at = (channel * count + k) * size
            mine, other = held[k * size : (k + 1) * size, :], taken_ref[at : at + size, :]
            one, two = jnp.where(lower, mine, other), jnp.where(lower, other, mine)
            at = channel * both
            out[at : at + cap, :] = one[:cap]
            if both > 2 * cap:
                out[at + cap : at + both - cap, :] = jnp.zeros((both - 2 * cap, LANES), jnp.float32)
            if shared:
                out[at + cap - shared : at + cap, :] = one[cap - shared : cap] + two[:shared]
            out[at + both - cap + shared : at + both, :] = two[shared:cap]
            if channel == 0:
                head = one[cap:] + two[cap:]
                if spilled is None:
                    over = jnp.maximum(head[lists + 1 : lists + 2] - both, 0.0)
                    spilled = head[lists : lists + 1] + jnp.sum(over, axis=1, keepdims=True)
                out[2 * both :, :] = jnp.where(line == lists, spilled, head)


def pack(me, held, taken, cap, both):
    count = held[0].shape[0] // (cap + HEAD)
    out = jax.ShapeDtypeStruct((2 * both + HEAD, taken.shape[1]), jnp.float32)
    return pl.pallas_call(
        functools.partial(pack_kernel, cap, both),
        in_specs=[SMEM] + [VMEM] * 3,
        out_specs=[VMEM] * count,
        out_shape=[out] * count,
        compiler_params=ROOM,
        name="pack",
    )(me, *held, taken)


def split(x):
    high = x.astype(jnp.bfloat16)
    return high, (x - high.astype(jnp.float32)).astype(jnp.bfloat16)


def collect_kernel(count, sub_tiles, me_ref, kept_ref, *refs):
    messages, keeps, (give_ref, *rows_s) = refs[:count], refs[count : count + SUBS], refs[count + SUBS :]
    both, pixels = (kept_ref.shape[0] - HEAD) // 2, kept_ref.shape[1]
    lists = -(-both // LANES)
    lower = me_ref[2] == 0
    flag = jnp.zeros((HEAD, pixels), jnp.float32)
    ids = []
    for i, (message, rows) in enumerate(zip(messages, rows_s)):
        whole = message[...]
        if i == 0:
            whole = jnp.where(lower, kept_ref[...], whole)
        rows[...] = jnp.concatenate([*split(whole[:both]), *split(whole[both : 2 * both])], axis=1)
        head = whole[2 * both :]
        flag = flag + head[lists : lists + 1]
        names = jnp.concatenate([head[n : n + 1] for n in range(lists)], axis=1)[:, :both]
        ids.append(names.astype(jnp.int32) - 1)
    chunk = min(256, sub_tiles)
    for sub, keep_ref in enumerate(keeps):
        at = sub * (sub_tiles + HEAD)
        for t in range(0, sub_tiles, chunk):
            sums = jnp.zeros((chunk, 4 * pixels), jnp.float32)
            for names, rows in zip(ids, rows_s):
                hit = ones_where(iota((chunk, both), 0) + (sub * sub_tiles + t) == names)
                sums = sums + dot(hit, rows[...])
            thermal = sums[:, :pixels] + sums[:, pixels : 2 * pixels]
            kinetic = sums[:, 2 * pixels : 3 * pixels] + sums[:, 3 * pixels :]
            keep_ref[t : t + chunk, :] = jnp.where(lower, thermal, kinetic)
            give_ref[at + t : at + t + chunk, :] = jnp.where(lower, kinetic, thermal)
        keep_ref[sub_tiles:, :] = flag
        give_ref[at + sub_tiles : at + sub_tiles + HEAD, :] = flag


def collect(me, kept, messages, sub_tiles):
    rows, pixels = kept.shape
    out = jax.ShapeDtypeStruct((sub_tiles + HEAD, pixels), jnp.float32)
    return pl.pallas_call(
        functools.partial(collect_kernel, len(messages), sub_tiles),
        in_specs=[SMEM] + [VMEM] * (1 + len(messages)),
        out_specs=[VMEM] * (SUBS + 1),
        out_shape=[out] * SUBS + [jax.ShapeDtypeStruct((SUBS * (sub_tiles + HEAD), pixels), jnp.float32)],
        scratch_shapes=[pltpu.VMEM(((rows - HEAD) // 2, 4 * pixels), jnp.bfloat16)] * len(messages),
        compiler_params=ROOM,
        name="collect",
    )(me, kept, *messages)


def owner_kernel(parts, me_ref, owner_ref, row_ref):
    most = row_ref.shape[1]
    owners = owner_ref[...]
    rows = owners.shape[0]
    mine = owners == me_ref[1] * 2 + me_ref[2]
    marks = jnp.where(mine, 1.0, 0.0)
    rank = running_counts(marks.astype(jnp.bfloat16), rows).astype(jnp.int32) - 1
    index = iota((rows, LANES), 0) * LANES + iota((rows, LANES), 1)
    found = jnp.zeros((HEAD, most), jnp.float32)
    line = iota((HEAD, LANES), 0)
    high, low = bytes_of(index + 1)
    for r in range(rows):
        pieces = jnp.where(line == 0, high[r : r + 1], jnp.where(line == 1, low[r : r + 1], 0.0))
        pieces = jnp.where(mine[r : r + 1], pieces, 0.0)
        spots = ones_where(iota((most, LANES), 0) == rank[r : r + 1])
        found = found + nt_dot(pieces.astype(jnp.bfloat16), spots)
    tile = (found[0:1] * 256.0 + found[1:2]).astype(jnp.int32) - 1
    tile = jnp.where(tile < 0, rows * LANES, tile)
    bounds = jnp.zeros((1, most), jnp.float32)
    for p in range(1, SUBS * parts + 1):
        before = jnp.where(index < p * (rows * LANES // (SUBS * parts)), marks, 0.0)
        bounds = jnp.where(iota((1, most), 1) == p, jnp.sum(before, axis=(0, 1), keepdims=True), bounds)
    row_ref[...] = jnp.where(iota((HEAD, most), 0) == 0, tile, bounds.astype(jnp.int32))


def owned_rows(me, owners, most, parts):
    return pl.pallas_call(
        functools.partial(owner_kernel, parts),
        in_specs=[SMEM, VMEM],
        out_specs=VMEM,
        out_shape=jax.ShapeDtypeStruct((HEAD, most), jnp.int32),
        compiler_params=ROOM,
        name="owned_rows",
    )(me, owners)


def fill_rows(row_ref, moves, start, end, shift):
    unroll = 8

    def one(r):
        at = pl.ds(row_ref[r] - shift, 1)
        for table, rows in moves:
            rows[pl.ds(r, 1), :] = table[at, :]

    def group(i, carry):
        for u in range(unroll):
            one(start + i * unroll + u)
        return carry

    def rest(r, carry):
        one(r)
        return carry

    groups = (end - start) // unroll
    lax.fori_loop(0, groups, group, 0)
    lax.fori_loop(start + groups * unroll, end, rest, 0)


def fill_part(m, sub, me_ref, row_ref, moves):
    most = moves[0][1].shape[0]
    tiles = moves[0][0].shape[0] - HEAD
    at = (me_ref[1] ^ m) * SUBS + sub
    fill_rows(row_ref, moves, row_ref[most + at], row_ref[most + at + 1], at * tiles)


def early_kernel(me_ref, row_ref, *refs):
    pieces, (own_rows, other_rows, flag_ref) = refs[:-3], refs[-3:]
    own, other = pieces[:SUBS], pieces[SUBS:]
    tiles = own[0].shape[0] - HEAD
    flag_ref[0] = jnp.max(own[0][tiles:, :]).astype(jnp.int32)
    own_rows[...] = jnp.zeros_like(own_rows)
    other_rows[...] = jnp.zeros_like(other_rows)
    for sub in range(SUBS):
        fill_part(0, sub, me_ref, row_ref, ((own[sub], own_rows), (other[sub], other_rows)))


def early(me, rows, own, other, most):
    out = jax.ShapeDtypeStruct((most, own[0].shape[1]), jnp.float32)
    return pl.pallas_call(
        early_kernel,
        in_specs=[SMEM, SMEM] + [VMEM] * (2 * SUBS),
        out_specs=[VMEM, VMEM, SMEM],
        out_shape=[out, out, jax.ShapeDtypeStruct((1,), jnp.int32)],
        compiler_params=ROOM,
        name="early",
    )(me, rows, *own, *other)


def middle_kernel(me_ref, row_ref, before_ref, *refs):
    pieces, rows_ref = refs[:-1], refs[-1]
    rows_ref[...] = before_ref[...]
    for i, piece in enumerate(pieces):
        fill_part(1 + i // SUBS, i % SUBS, me_ref, row_ref, ((piece, rows_ref),))


def middle(me, rows, before, pieces):
    return pl.pallas_call(
        middle_kernel,
        in_specs=[SMEM, SMEM, VMEM] + [VMEM] * len(pieces),
        out_specs=VMEM,
        out_shape=jax.ShapeDtypeStruct(before.shape, jnp.float32),
        compiler_params=ROOM,
        name="middle",
    )(me, rows, before, *pieces)


def late_kernel(me_ref, row_ref, own_rows, before_ref, *refs):
    pieces, (owned_ref, map_ref, other_rows) = refs[:-3], refs[-3:]
    tiles, pixels = pieces[0].shape[0] - HEAD, pieces[0].shape[1]
    half = len(pieces) // 2
    lower = me_ref[2] == 0

    def put(ref, at, own, other):
        ref[at, :pixels] = jnp.where(lower, own, other)
        ref[at, pixels:] = jnp.where(lower, other, own)

    other_rows[...] = before_ref[...]
    for i in range(half):
        own, other = pieces[i], pieces[half + i]
        m, sub = i // SUBS, i % SUBS
        at = pl.multiple_of(((me_ref[1] ^ m) * SUBS + sub) * tiles, tiles)
        put(map_ref, pl.ds(at, tiles), own[:tiles, :], other[:tiles, :])
        if m:
            fill_part(m, sub, me_ref, row_ref, ((other, other_rows),))
    put(owned_ref, slice(None), own_rows[...], other_rows[...])


def late(me, rows, own_rows, before, own, other, block):
    most, pixels = own_rows.shape
    return pl.pallas_call(
        late_kernel,
        in_specs=[SMEM, SMEM] + [VMEM] * (2 + len(own) + len(other)),
        out_specs=[VMEM, VMEM],
        out_shape=[
            jax.ShapeDtypeStruct((most, 2 * pixels), jnp.float32),
            jax.ShapeDtypeStruct((block, 2 * pixels), jnp.float32),
        ],
        scratch_shapes=[pltpu.VMEM((most, pixels), jnp.float32)],
        compiler_params=ROOM,
        name="late",
    )(me, rows, own_rows, before, *own, *other)


def shards(kernel, pressure, velocity, entry_slot, slot_tile, tile_owner):
    vols = lax.axis_size("vol")
    pixs = lax.axis_size("pix")
    vol = lax.axis_index("vol")
    pix = lax.axis_index("pix")
    entries, _ = kernel.shape
    slots = slot_tile.shape[1]
    block = tile_owner.shape[0] // vols
    parts = pixs // 2
    part_tiles = block // parts
    half = vols // 2
    most_owned = 2 * block // pixs
    most_rows = min(2 * slots // vols, part_tiles)
    me = jnp.stack([vol, pix >> 1, pix & 1]).astype(jnp.int32)
    tiles = slot_tile.reshape(slots // LANES, LANES)
    slot = entry_slot.reshape(entries // LANES, LANES)
    factors = [x.reshape(entries // LANES, LANES) for x in (pressure, velocity)]
    owners = lax.dynamic_slice_in_dim(
        tile_owner.reshape(vols, block // LANES, LANES), vol, 1
    )[0]
    rows = owned_rows(me, owners, most_owned, parts)[:2].reshape(-1)

    def send(x, vol_step=0, part_step=0, core_step=0):
        step = (vol_step * parts + part_step) * 2 + core_step
        return lax.ppermute(x, ("vol", "pix"), [(d, d ^ step) for d in range(vols * pixs)])

    def exchange(cap, both):
        count = half * parts
        quarter = count // 2
        order = class_order(count)
        sub_rows = part_tiles // SUBS + HEAD
        place, ends, head = plan(me, tiles, slot, vols, parts, block, cap, both)
        *held, given = project(
            me, kernel, factors, slot, ends.reshape(-1), place.reshape(-1), head, cap
        )
        messages = pack(me, held, send(given, core_step=1), cap, both)

        def gather(messages):
            arrived = [None] * quarter
            for j in reversed(range(quarter)):
                steps = [order[(d & 1) * quarter + j] for d in range(vols * pixs)]
                pairs = [(d, d ^ (step << 1)) for d, step in enumerate(steps) if step]
                arrived[j] = lax.ppermute(messages[j], ("vol", "pix"), pairs)
            *keeps, give = collect(me, messages[0], arrived, part_tiles // SUBS)
            taken = send(give, core_step=1)
            sums = [x + taken[i * sub_rows : (i + 1) * sub_rows] for i, x in enumerate(keeps)]
            return lax.optimization_barrier(sums)

        far = gather(messages[quarter:])
        crossed = [send(x, vol_step=half) for x in far]
        near = gather(messages[:quarter])
        mine = [x + y for x, y in zip(near, crossed)]
        other = [send(x, core_step=1) for x in mine]
        own_rows, other_rows, flag = early(me, rows, mine, other, most_owned)
        across = [send(x, part_step=m) for m in range(1, parts) for x in mine]
        beyond = [send(x, core_step=1) for x in across]
        own_rows = middle(me, rows, own_rows, across)
        full = late(me, rows, own_rows, other_rows, mine + across, other + beyond, block)
        return flag[0] > 0, *full

    def rows_of(share):
        return most_rows * share // 32 // 8 * 8

    result = exchange(rows_of(13), rows_of(24))

    def redo(state):
        unused, *full = exchange(most_rows, 2 * most_rows)
        return jnp.zeros((), bool), *full

    _, owned, shell = lax.while_loop(lambda state: state[0], redo, result)
    return owned, shell


def solution(mesh):
    in_specs = (
        P(("vol", "pix"), None),
        P(("vol", "pix")),
        P(("vol", "pix")),
        P(("vol", "pix"), None),
        P(("vol", "pix"), None),
        P(),
    )
    out_specs = (P(("vol", "pix"), None), P("vol", None))
    return jax.shard_map(shards, mesh=mesh, in_specs=in_specs, out_specs=out_specs, check_vma=False)
```

```python
import functools

import jax
import jax.numpy as jnp
from jax import lax
from jax.experimental import pallas as pl
from jax.experimental.pallas import tpu as pltpu
from jax.sharding import PartitionSpec as P


LANES = 128
HEAD = 8
ROOM = pltpu.CompilerParams(vmem_limit_bytes=16 << 20)
GROUP = 256
WINDOW = 40
SUBS = 2


SMEM = pl.BlockSpec(memory_space=pltpu.SMEM)
VMEM = pl.BlockSpec(memory_space=pltpu.VMEM)
ANY = pl.BlockSpec(memory_space=pl.ANY)
HBM = pl.BlockSpec(memory_space=pltpu.HBM)


def iota(shape, axis):
    return lax.broadcasted_iota(jnp.int32, shape, axis)


def nt_dot(a, b):
    return lax.dot_general(a, b, (((1,), (1,)), ((), ())), preferred_element_type=jnp.float32)


def dot(a, b):
    return jnp.dot(a, b, preferred_element_type=jnp.float32)


def ones_where(mask):
    return jnp.where(mask, 1.0, 0.0).astype(jnp.bfloat16)


def bytes_of(x):
    return (x >> 8).astype(jnp.float32), (x & 255).astype(jnp.float32)


def running_counts(marks, rows):
    total = marks.shape[0]
    upper = ones_where(iota((LANES, LANES), 0) <= iota((LANES, LANES), 1))
    row, column = iota((total, total), 0), iota((total, total), 1)
    earlier = ones_where((column < row) & (row // rows == column // rows))
    before = dot(earlier, marks).astype(jnp.bfloat16)
    return dot(marks, upper) + dot(before, jnp.ones((LANES, LANES), jnp.bfloat16))


def plan_kernel(vols, parts, block, cap, both, me_ref, tile_ref, slot_ref, place_ref, ends_ref, head_ref):
    size = cap + HEAD
    part_tiles = block // parts
    lane = iota((HEAD, LANES), 1)
    line = iota((HEAD, LANES), 0)
    slots = slot_ref[...]
    ends = ones_where(((line == 0) & (lane == 0)) | ((line == 1) & (lane == LANES - 1)))
    high, low = bytes_of(slots)
    ends_ref[...] = (
        nt_dot(ends, high.astype(jnp.bfloat16)) * 256.0 + nt_dot(ends, low.astype(jnp.bfloat16))
    ).astype(jnp.int32)

    tiles = tile_ref[...]
    rows = tiles.shape[0]
    classes = vols * parts
    part = tiles // part_tiles
    group = part ^ (me_ref[0] * parts + me_ref[1])
    marks = jnp.concatenate([jnp.where(group == i, 1.0, 0.0) for i in range(classes)], axis=0)
    counts = running_counts(marks.astype(jnp.bfloat16), rows) * marks
    place = jnp.zeros((rows, LANES), jnp.float32)
    for i in range(classes):
        place = place + counts[i * rows : (i + 1) * rows]
    place = place.astype(jnp.int32) - 1
    fits = place < cap
    spilled = jnp.sum(jnp.where(fits, 0.0, 1.0), axis=(0, 1), keepdims=True)
    place = jnp.where(me_ref[2] == 0, place, cap - 1 - place)
    place_ref[...] = jnp.where(fits, group * size + place, classes * size)
    lists = -(-both // LANES)
    width = lists * LANES
    spot = jnp.where(fits, place + me_ref[2] * (both - cap), -1)
    high, low = bytes_of(tiles - part * part_tiles + 1)
    ids = jnp.zeros((2 * classes, width), jnp.float32)
    which = iota((classes, LANES), 0)
    for r in range(rows):
        here = group[r : r + 1] == which
        pieces = jnp.concatenate(
            [jnp.where(here, high[r : r + 1], 0.0), jnp.where(here, low[r : r + 1], 0.0)], axis=0
        )
        spots = ones_where(iota((width, LANES), 0) == spot[r : r + 1])
        ids = ids + nt_dot(pieces.astype(jnp.bfloat16), spots)
    ids = ids[:classes] * 256.0 + ids[classes:]
    for k in range(classes):
        held = jnp.max(counts[k * rows : (k + 1) * rows], axis=(0, 1), keepdims=True)
        head = jnp.where(line == lists, jnp.broadcast_to(spilled, (HEAD, LANES)), 0.0)
        head = jnp.where(line == lists + 1, jnp.broadcast_to(held, (HEAD, LANES)), head)
        for i in range(lists):
            head = jnp.where(line == i, ids[k : k + 1, i * LANES : (i + 1) * LANES], head)
        head_ref[k * HEAD : (k + 1) * HEAD, :] = head


def plan(me, tiles, slot, vols, parts, block, cap, both):
    rows = tiles.shape[0]
    return pl.pallas_call(
        functools.partial(plan_kernel, vols, parts, block, cap, both),
        in_specs=[SMEM, VMEM, VMEM],
        out_specs=[VMEM, VMEM, VMEM],
        out_shape=[
            jax.ShapeDtypeStruct((rows, LANES), jnp.int32),
            jax.ShapeDtypeStruct((HEAD, slot.shape[0]), jnp.int32),
            jax.ShapeDtypeStruct((vols * parts * HEAD, LANES), jnp.float32),
        ],
        compiler_params=ROOM,
        name="plan",
    )(me, tiles, slot)


def project_kernel(
    steps, cap, me_ref, ends_ref, place_ref, kernel_hbm, thermal_ref, kinetic_ref, slot_ref, head_ref,
    own_out, other_out,
    kernel_ref, own_ref, other_ref, own_stage, other_stage, own_s, other_s, in_sem
):
    entries, _ = kernel_ref.shape
    part = entries // steps
    groups = part // GROUP
    lines = GROUP // LANES
    slots = place_ref.shape[0]
    total = entries // LANES

    def load(step):
        piece = pl.ds(pl.multiple_of(step * part, part), part)
        return pltpu.make_async_copy(kernel_hbm.at[piece], kernel_ref.at[piece], in_sem.at[step])

    for step in range(steps):
        load(step).start()
    for ref in (own_ref, other_ref, own_stage, other_stage):
        ref[...] = jnp.zeros_like(ref)
    thermal, kinetic = thermal_ref[...].astype(jnp.float32), kinetic_ref[...].astype(jnp.float32)
    own_s[...] = jnp.where(me_ref[2] == 0, thermal, kinetic)
    other_s[...] = jnp.where(me_ref[2] == 0, kinetic, thermal)
    line = iota((WINDOW, LANES), 0)

    def first(group):
        return ends_ref[group * lines] & -8

    def reach(group):
        return ends_ref[total + group * lines + lines - 1] - first(group)

    def add(group, base):
        own, other = [], []
        for r in range(lines):
            at = pl.ds(group * lines + r, 1)
            match = line == slot_ref[at, :] - base
            own.append(jnp.where(match, own_s[at, :], 0.0))
            other.append(jnp.where(match, other_s[at, :], 0.0))
        weights = jnp.concatenate(
            [jnp.concatenate(own, axis=1), jnp.concatenate(other, axis=1)], axis=0
        ).astype(jnp.bfloat16)
        sums = dot(weights, kernel_ref[pl.ds(pl.multiple_of(group * GROUP, GROUP), GROUP), :])
        window = pl.ds(pl.multiple_of(base, 8), WINDOW)
        own_ref[window, :] += sums[:WINDOW]
        other_ref[window, :] += sums[WINDOW:]

    def turn(step, most):
        load(step).wait()
        for g in range(groups):
            group = step * groups + g
            add(group, first(group))
            most = jnp.maximum(most, reach(group))
        return most

    most = lax.fori_loop(0, steps, turn, 0)

    @pl.when(most >= WINDOW)
    def _():
        def more(group, carry):
            def again(w, inner):
                add(group, first(group) + w * WINDOW)
                return inner

            return lax.fori_loop(1, reach(group) // WINDOW + 1, again, carry)

        lax.fori_loop(0, steps * groups, more, 0)

    unroll = 16

    def move(i, carry):
        for u in range(unroll):
            s = i * unroll + u
            to = place_ref[s]
            own_stage[pl.ds(to, 1), :] = own_ref[pl.ds(s, 1), :]
            other_stage[pl.ds(to, 1), :] = other_ref[pl.ds(s, 1), :]
        return carry

    lax.fori_loop(0, slots // unroll, move, 0)
    size = cap + HEAD
    for out, stage in ((own_out, own_stage), (other_out, other_stage)):
        for k in range(head_ref.shape[0] // HEAD):
            at = k * size
            out[at : at + cap, :] = stage[at : at + cap, :]
            out[at + cap : at + size, :] = head_ref[k * HEAD : (k + 1) * HEAD, :]


def project(me, kernel, factors, slot, ends, place, head, cap):
    entries, pixels = kernel.shape
    slots = place.shape[0]
    steps = 4
    rows = head.shape[0] // HEAD * (cap + HEAD)
    partial = pltpu.VMEM((slots + WINDOW, pixels), jnp.float32)
    stage = pltpu.VMEM((rows + HEAD, pixels), jnp.float32)
    factor = pltpu.VMEM(slot.shape, jnp.float32)
    return pl.pallas_call(
        functools.partial(project_kernel, steps, cap),
        in_specs=[SMEM, SMEM, SMEM, HBM, VMEM, VMEM, VMEM, VMEM],
        out_specs=[VMEM] * 2,
        out_shape=[jax.ShapeDtypeStruct((rows, pixels), jnp.float32)] * 2,
        scratch_shapes=[
            pltpu.VMEM((entries, pixels), kernel.dtype),
            partial, partial, stage, stage, factor, factor,
            pltpu.SemaphoreType.DMA((steps,)),
        ],
        compiler_params=ROOM,
        name="project",
    )(me, ends, place, kernel, *factors, slot, head)


def pack_kernel(cap, both, me_ref, mine_ref, other_ref, *outs):
    size = cap + HEAD
    lists = -(-both // LANES)
    lower = me_ref[2] == 0
    line = iota((HEAD, LANES), 0)
    heads, spilled = [], jnp.zeros((1, LANES), jnp.float32)
    for k, out in enumerate(outs):
        mine, other = mine_ref[k * size : (k + 1) * size, :], other_ref[k * size : (k + 1) * size, :]
        one, two = jnp.where(lower, mine, other), jnp.where(lower, other, mine)
        out[:cap, :] = one[:cap]
        if both > 2 * cap:
            out[cap : both - cap, :] = jnp.zeros((both - 2 * cap, LANES), jnp.float32)
        shared = max(2 * cap - both, 0)
        if shared:
            out[cap - shared : cap, :] = one[cap - shared : cap] + two[:shared]
        out[cap + max(both - 2 * cap, 0) : both, :] = two[shared:cap]
        head = one[cap:] + two[cap:]
        heads.append(head)
        spilled = spilled + head[lists : lists + 1] + jnp.maximum(head[lists + 1 : lists + 2] - both, 0.0)
    for out, head in zip(outs, heads):
        out[both:, :] = jnp.where(line == lists, spilled, head)


def pack(me, mine, other, cap, both):
    count = mine.shape[0] // (cap + HEAD)
    out = jax.ShapeDtypeStruct((both + HEAD, mine.shape[1]), jnp.float32)
    return pl.pallas_call(
        functools.partial(pack_kernel, cap, both),
        in_specs=[SMEM, VMEM, VMEM],
        out_specs=[VMEM] * count,
        out_shape=[out] * count,
        compiler_params=ROOM,
        name="pack",
    )(me, mine, other)


def split(x):
    high = x.astype(jnp.bfloat16)
    return high, (x - high.astype(jnp.float32)).astype(jnp.bfloat16)


def collect_kernel(count, sub_tiles, *refs):
    messages, outs, rows_s = refs[:count], refs[count : count + SUBS], refs[count + SUBS :]
    both, pixels = messages[0].shape[0] - HEAD, messages[0].shape[1]
    lists = -(-both // LANES)
    flag = jnp.zeros((HEAD, pixels), jnp.float32)
    ids = []
    for message, rows in zip(messages, rows_s):
        rows[...] = jnp.concatenate(split(message[:both, :]), axis=1)
        head = message[both:, :]
        flag = flag + head[lists : lists + 1]
        names = jnp.concatenate([head[i : i + 1] for i in range(lists)], axis=1)[:, :both]
        ids.append(names.astype(jnp.int32) - 1)
    chunk = min(256, sub_tiles)
    for sub, out_ref in enumerate(outs):
        for t in range(0, sub_tiles, chunk):
            sums = jnp.zeros((chunk, 2 * pixels), jnp.float32)
            for names, rows in zip(ids, rows_s):
                hit = ones_where(iota((chunk, both), 0) + (sub * sub_tiles + t) == names)
                sums = sums + dot(hit, rows[...])
            out_ref[t : t + chunk, :] = sums[:, :pixels] + sums[:, pixels:]
        out_ref[sub_tiles:, :] = flag


def collect(messages, sub_tiles):
    rows, pixels = messages[0].shape
    return pl.pallas_call(
        functools.partial(collect_kernel, len(messages), sub_tiles),
        in_specs=[VMEM] * len(messages),
        out_specs=[VMEM] * SUBS,
        out_shape=[jax.ShapeDtypeStruct((sub_tiles + HEAD, pixels), jnp.float32)] * SUBS,
        scratch_shapes=[pltpu.VMEM((rows - HEAD, 2 * pixels), jnp.bfloat16)] * len(messages),
        compiler_params=ROOM,
        name="collect",
    )(*messages)


def owner_kernel(parts, me_ref, owner_ref, row_ref):
    most = row_ref.shape[1]
    owners = owner_ref[...]
    rows = owners.shape[0]
    mine = owners == me_ref[1] * 2 + me_ref[2]
    marks = jnp.where(mine, 1.0, 0.0)
    rank = running_counts(marks.astype(jnp.bfloat16), rows).astype(jnp.int32) - 1
    index = iota((rows, LANES), 0) * LANES + iota((rows, LANES), 1)
    found = jnp.zeros((HEAD, most), jnp.float32)
    line = iota((HEAD, LANES), 0)
    high, low = bytes_of(index + 1)
    for r in range(rows):
        pieces = jnp.where(line == 0, high[r : r + 1], jnp.where(line == 1, low[r : r + 1], 0.0))
        pieces = jnp.where(mine[r : r + 1], pieces, 0.0)
        spots = ones_where(iota((most, LANES), 0) == rank[r : r + 1])
        found = found + nt_dot(pieces.astype(jnp.bfloat16), spots)
    tile = (found[0:1] * 256.0 + found[1:2]).astype(jnp.int32) - 1
    tile = jnp.where(tile < 0, rows * LANES, tile)
    bounds = jnp.zeros((1, most), jnp.float32)
    for p in range(1, SUBS * parts + 1):
        before = jnp.where(index < p * (rows * LANES // (SUBS * parts)), marks, 0.0)
        bounds = jnp.where(iota((1, most), 1) == p, jnp.sum(before, axis=(0, 1), keepdims=True), bounds)
    row_ref[...] = jnp.where(iota((HEAD, most), 0) == 0, tile, bounds.astype(jnp.int32))


def owned_rows(me, owners, most, parts):
    return pl.pallas_call(
        functools.partial(owner_kernel, parts),
        in_specs=[SMEM, VMEM],
        out_specs=VMEM,
        out_shape=jax.ShapeDtypeStruct((HEAD, most), jnp.int32),
        compiler_params=ROOM,
        name="owned_rows",
    )(me, owners)


def fill_rows(row_ref, moves, start, end, shift):
    unroll = 8

    def one(r):
        at = pl.ds(row_ref[r] - shift, 1)
        for table, rows in moves:
            rows[pl.ds(r, 1), :] = table[at, :]

    def group(i, carry):
        for u in range(unroll):
            one(start + i * unroll + u)
        return carry

    def rest(r, carry):
        one(r)
        return carry

    groups = (end - start) // unroll
    lax.fori_loop(0, groups, group, 0)
    lax.fori_loop(start + groups * unroll, end, rest, 0)


def fill_part(m, sub, me_ref, row_ref, moves):
    most = moves[0][1].shape[0]
    tiles = moves[0][0].shape[0] - HEAD
    at = (me_ref[1] ^ m) * SUBS + sub
    fill_rows(row_ref, moves, row_ref[most + at], row_ref[most + at + 1], at * tiles)


def early_kernel(me_ref, row_ref, *refs):
    pieces, (own_rows, other_rows, flag_ref) = refs[:-3], refs[-3:]
    own, other = pieces[:SUBS], pieces[SUBS:]
    tiles = own[0].shape[0] - HEAD
    flag_ref[0] = jnp.max(own[0][tiles:, :]).astype(jnp.int32)
    own_rows[...] = jnp.zeros_like(own_rows)
    other_rows[...] = jnp.zeros_like(other_rows)
    for sub in range(SUBS):
        fill_part(0, sub, me_ref, row_ref, ((own[sub], own_rows), (other[sub], other_rows)))


def early(me, rows, own, other, most):
    out = jax.ShapeDtypeStruct((most, own[0].shape[1]), jnp.float32)
    return pl.pallas_call(
        early_kernel,
        in_specs=[SMEM, SMEM] + [VMEM] * (2 * SUBS),
        out_specs=[VMEM, VMEM, SMEM],
        out_shape=[out, out, jax.ShapeDtypeStruct((1,), jnp.int32)],
        compiler_params=ROOM,
        name="early",
    )(me, rows, *own, *other)


def middle_kernel(me_ref, row_ref, before_ref, *refs):
    pieces, rows_ref = refs[:-1], refs[-1]
    rows_ref[...] = before_ref[...]
    for i, piece in enumerate(pieces):
        fill_part(1 + i // SUBS, i % SUBS, me_ref, row_ref, ((piece, rows_ref),))


def middle(me, rows, before, pieces):
    return pl.pallas_call(
        middle_kernel,
        in_specs=[SMEM, SMEM, VMEM] + [VMEM] * len(pieces),
        out_specs=VMEM,
        out_shape=jax.ShapeDtypeStruct(before.shape, jnp.float32),
        compiler_params=ROOM,
        name="middle",
    )(me, rows, before, *pieces)


def late_kernel(me_ref, row_ref, own_rows, before_ref, *refs):
    pieces, (owned_ref, map_ref, other_rows) = refs[:-3], refs[-3:]
    tiles, pixels = pieces[0].shape[0] - HEAD, pieces[0].shape[1]
    half = len(pieces) // 2
    lower = me_ref[2] == 0

    def put(ref, at, own, other):
        ref[at, :pixels] = jnp.where(lower, own, other)
        ref[at, pixels:] = jnp.where(lower, other, own)

    other_rows[...] = before_ref[...]
    for i in range(half):
        own, other = pieces[i], pieces[half + i]
        m, sub = i // SUBS, i % SUBS
        at = pl.multiple_of(((me_ref[1] ^ m) * SUBS + sub) * tiles, tiles)
        put(map_ref, pl.ds(at, tiles), own[:tiles, :], other[:tiles, :])
        if m:
            fill_part(m, sub, me_ref, row_ref, ((other, other_rows),))
    put(owned_ref, slice(None), own_rows[...], other_rows[...])


def late(me, rows, own_rows, before, own, other, block):
    most, pixels = own_rows.shape
    return pl.pallas_call(
        late_kernel,
        in_specs=[SMEM, SMEM] + [VMEM] * (2 + len(own) + len(other)),
        out_specs=[VMEM, VMEM],
        out_shape=[
            jax.ShapeDtypeStruct((most, 2 * pixels), jnp.float32),
            jax.ShapeDtypeStruct((block, 2 * pixels), jnp.float32),
        ],
        scratch_shapes=[pltpu.VMEM((most, pixels), jnp.float32)],
        compiler_params=ROOM,
        name="late",
    )(me, rows, own_rows, before, *own, *other)


def shards(kernel, pressure, velocity, entry_slot, slot_tile, tile_owner):
    vols = lax.axis_size("vol")
    pixs = lax.axis_size("pix")
    vol = lax.axis_index("vol")
    pix = lax.axis_index("pix")
    entries, _ = kernel.shape
    slots = slot_tile.shape[1]
    block = tile_owner.shape[0] // vols
    parts = pixs // 2
    part_tiles = block // parts
    half = vols // 2
    most_owned = 2 * block // pixs
    most_rows = min(2 * slots // vols, part_tiles)
    me = jnp.stack([vol, pix >> 1, pix & 1]).astype(jnp.int32)
    tiles = slot_tile.reshape(slots // LANES, LANES)
    slot = entry_slot.reshape(entries // LANES, LANES)
    factors = [x.reshape(entries // LANES, LANES) for x in (pressure, velocity)]
    owners = lax.dynamic_slice_in_dim(
        tile_owner.reshape(vols, block // LANES, LANES), vol, 1
    )[0]
    rows = owned_rows(me, owners, most_owned, parts)[:2].reshape(-1)

    def send(x, vol_step=0, part_step=0, core_step=0):
        step = (vol_step * parts + part_step) * 2 + core_step
        return lax.ppermute(x, ("vol", "pix"), [(d, d ^ step) for d in range(vols * pixs)])

    def exchange(cap, both):
        count = half * parts
        place, ends, head = plan(me, tiles, slot, vols, parts, block, cap, both)
        own, given = project(
            me, kernel, factors, slot, ends.reshape(-1), place.reshape(-1), head, cap
        )
        messages = pack(me, own, send(given, core_step=1), cap, both)

        def gather(messages):
            messages = list(messages)
            for k in reversed(range(1, count)):
                messages[k] = send(messages[k], k // parts, k % parts)
            return collect(messages, part_tiles // SUBS)

        far = gather(messages[count:])
        crossed = [send(x, vol_step=half) for x in far]
        near = gather(messages[:count])
        mine = [x + y for x, y in zip(near, crossed)]
        other = [send(x, core_step=1) for x in mine]
        own_rows, other_rows, flag = early(me, rows, mine, other, most_owned)
        across = [send(x, part_step=m) for m in range(1, parts) for x in mine]
        beyond = [send(x, core_step=1) for x in across]
        own_rows = middle(me, rows, own_rows, across)
        full = late(me, rows, own_rows, other_rows, mine + across, other + beyond, block)
        return flag[0] > 0, *full

    def rows_of(share):
        return most_rows * share // 32 // 8 * 8

    result = exchange(rows_of(13), rows_of(24))

    def redo(state):
        unused, *full = exchange(most_rows, 2 * most_rows)
        return jnp.zeros((), bool), *full

    _, owned, shell = lax.while_loop(lambda state: state[0], redo, result)
    return owned, shell


def solution(mesh):
    in_specs = (
        P(("vol", "pix"), None),
        P(("vol", "pix")),
        P(("vol", "pix")),
        P(("vol", "pix"), None),
        P(("vol", "pix"), None),
        P(),
    )
    out_specs = (P(("vol", "pix"), None), P("vol", None))
    return jax.shard_map(shards, mesh=mesh, in_specs=in_specs, out_specs=out_specs, check_vma=False)
```

```python
import functools

import jax
import jax.numpy as jnp
from jax import lax
from jax.experimental import pallas as pl
from jax.experimental.pallas import tpu as pltpu
from jax.sharding import PartitionSpec as P


LANES = 128
HEAD = 8
ROOM = pltpu.CompilerParams(vmem_limit_bytes=16 << 20)
GROUP = 256
WINDOW = 40
SUBS = 2


SMEM = pl.BlockSpec(memory_space=pltpu.SMEM)
VMEM = pl.BlockSpec(memory_space=pltpu.VMEM)
ANY = pl.BlockSpec(memory_space=pl.ANY)
HBM = pl.BlockSpec(memory_space=pltpu.HBM)


def iota(shape, axis):
    return lax.broadcasted_iota(jnp.int32, shape, axis)


def nt_dot(a, b):
    return lax.dot_general(a, b, (((1,), (1,)), ((), ())), preferred_element_type=jnp.float32)


def dot(a, b):
    return jnp.dot(a, b, preferred_element_type=jnp.float32)


def ones_where(mask):
    return jnp.where(mask, 1.0, 0.0).astype(jnp.bfloat16)


def bytes_of(x):
    return (x >> 8).astype(jnp.float32), (x & 255).astype(jnp.float32)


def running_counts(marks, rows):
    total = marks.shape[0]
    upper = ones_where(iota((LANES, LANES), 0) <= iota((LANES, LANES), 1))
    row, column = iota((total, total), 0), iota((total, total), 1)
    earlier = ones_where((column < row) & (row // rows == column // rows))
    before = dot(earlier, marks).astype(jnp.bfloat16)
    return dot(marks, upper) + dot(before, jnp.ones((LANES, LANES), jnp.bfloat16))


def plan_kernel(vols, parts, block, cap, both, me_ref, tile_ref, slot_ref, place_ref, ends_ref, head_ref):
    size = cap + HEAD
    part_tiles = block // parts
    lane = iota((HEAD, LANES), 1)
    line = iota((HEAD, LANES), 0)
    slots = slot_ref[...]
    ends = ones_where(((line == 0) & (lane == 0)) | ((line == 1) & (lane == LANES - 1)))
    high, low = bytes_of(slots)
    ends_ref[...] = (
        nt_dot(ends, high.astype(jnp.bfloat16)) * 256.0 + nt_dot(ends, low.astype(jnp.bfloat16))
    ).astype(jnp.int32)

    tiles = tile_ref[...]
    rows = tiles.shape[0]
    classes = vols * parts
    part = tiles // part_tiles
    group = part ^ (me_ref[0] * parts + me_ref[1])
    marks = jnp.concatenate([jnp.where(group == i, 1.0, 0.0) for i in range(classes)], axis=0)
    counts = running_counts(marks.astype(jnp.bfloat16), rows) * marks
    place = jnp.zeros((rows, LANES), jnp.float32)
    for i in range(classes):
        place = place + counts[i * rows : (i + 1) * rows]
    place = place.astype(jnp.int32) - 1
    fits = place < cap
    spilled = jnp.sum(jnp.where(fits, 0.0, 1.0), axis=(0, 1), keepdims=True)
    place = jnp.where(me_ref[2] == 0, place, cap - 1 - place)
    place_ref[...] = jnp.where(fits, group * size + place, classes * size - 1)
    lists = -(-both // LANES)
    width = lists * LANES
    spot = jnp.where(fits, place + me_ref[2] * (both - cap), -1)
    high, low = bytes_of(tiles - part * part_tiles + 1)
    ids = jnp.zeros((2 * classes, width), jnp.float32)
    which = iota((classes, LANES), 0)
    for r in range(rows):
        here = group[r : r + 1] == which
        pieces = jnp.concatenate(
            [jnp.where(here, high[r : r + 1], 0.0), jnp.where(here, low[r : r + 1], 0.0)], axis=0
        )
        spots = ones_where(iota((width, LANES), 0) == spot[r : r + 1])
        ids = ids + nt_dot(pieces.astype(jnp.bfloat16), spots)
    ids = ids[:classes] * 256.0 + ids[classes:]
    for k in range(classes):
        held = jnp.max(counts[k * rows : (k + 1) * rows], axis=(0, 1), keepdims=True)
        head = jnp.where(line == lists, jnp.broadcast_to(spilled, (HEAD, LANES)), 0.0)
        head = jnp.where(line == lists + 1, jnp.broadcast_to(held, (HEAD, LANES)), head)
        for i in range(lists):
            head = jnp.where(line == i, ids[k : k + 1, i * LANES : (i + 1) * LANES], head)
        head_ref[k * HEAD : (k + 1) * HEAD, :] = head


def plan(me, tiles, slot, vols, parts, block, cap, both):
    rows = tiles.shape[0]
    return pl.pallas_call(
        functools.partial(plan_kernel, vols, parts, block, cap, both),
        in_specs=[SMEM, VMEM, VMEM],
        out_specs=[VMEM, VMEM, VMEM],
        out_shape=[
            jax.ShapeDtypeStruct((rows, LANES), jnp.int32),
            jax.ShapeDtypeStruct((HEAD, slot.shape[0]), jnp.int32),
            jax.ShapeDtypeStruct((vols * parts * HEAD, LANES), jnp.float32),
        ],
        compiler_params=ROOM,
        name="plan",
    )(me, tiles, slot)


def project_kernel(
    steps, cap, me_ref, ends_ref, place_ref, kernel_hbm, thermal_ref, kinetic_ref, slot_ref, head_ref,
    own_out, other_out,
    kernel_ref, own_ref, other_ref, own_s, other_s, in_sem
):
    entries, _ = kernel_ref.shape
    part = entries // steps
    groups = part // GROUP
    lines = GROUP // LANES
    slots = place_ref.shape[0]
    total = entries // LANES

    def load(step):
        piece = pl.ds(pl.multiple_of(step * part, part), part)
        return pltpu.make_async_copy(kernel_hbm.at[piece], kernel_ref.at[piece], in_sem.at[step])

    for step in range(steps):
        load(step).start()
    for ref in (own_ref, other_ref, own_out, other_out):
        ref[...] = jnp.zeros_like(ref)
    thermal, kinetic = thermal_ref[...].astype(jnp.float32), kinetic_ref[...].astype(jnp.float32)
    own_s[...] = jnp.where(me_ref[2] == 0, thermal, kinetic)
    other_s[...] = jnp.where(me_ref[2] == 0, kinetic, thermal)
    line = iota((WINDOW, LANES), 0)

    def first(group):
        return ends_ref[group * lines] & -8

    def reach(group):
        return ends_ref[total + group * lines + lines - 1] - first(group)

    def add(group, base):
        own, other = [], []
        for r in range(lines):
            at = pl.ds(group * lines + r, 1)
            match = line == slot_ref[at, :] - base
            own.append(jnp.where(match, own_s[at, :], 0.0))
            other.append(jnp.where(match, other_s[at, :], 0.0))
        weights = jnp.concatenate(
            [jnp.concatenate(own, axis=1), jnp.concatenate(other, axis=1)], axis=0
        ).astype(jnp.bfloat16)
        sums = dot(weights, kernel_ref[pl.ds(pl.multiple_of(group * GROUP, GROUP), GROUP), :])
        window = pl.ds(pl.multiple_of(base, 8), WINDOW)
        own_ref[window, :] += sums[:WINDOW]
        other_ref[window, :] += sums[WINDOW:]

    def turn(step, most):
        load(step).wait()
        for g in range(groups):
            group = step * groups + g
            add(group, first(group))
            most = jnp.maximum(most, reach(group))
        return most

    most = lax.fori_loop(0, steps, turn, 0)

    @pl.when(most >= WINDOW)
    def _():
        def more(group, carry):
            def again(w, inner):
                add(group, first(group) + w * WINDOW)
                return inner

            return lax.fori_loop(1, reach(group) // WINDOW + 1, again, carry)

        lax.fori_loop(0, steps * groups, more, 0)

    unroll = 16

    def move(i, carry):
        for u in range(unroll):
            s = i * unroll + u
            to = place_ref[s]
            own_out[pl.ds(to, 1), :] = own_ref[pl.ds(s, 1), :]
            other_out[pl.ds(to, 1), :] = other_ref[pl.ds(s, 1), :]
        return carry

    lax.fori_loop(0, slots // unroll, move, 0)
    size = cap + HEAD
    for out in (own_out, other_out):
        for k in range(head_ref.shape[0] // HEAD):
            at = k * size
            out[at + cap : at + size, :] = head_ref[k * HEAD : (k + 1) * HEAD, :]


def project(me, kernel, factors, slot, ends, place, head, cap):
    entries, pixels = kernel.shape
    slots = place.shape[0]
    steps = 4
    rows = head.shape[0] // HEAD * (cap + HEAD)
    partial = pltpu.VMEM((slots + WINDOW, pixels), jnp.float32)
    factor = pltpu.VMEM(slot.shape, jnp.float32)
    return pl.pallas_call(
        functools.partial(project_kernel, steps, cap),
        in_specs=[SMEM, SMEM, SMEM, HBM, VMEM, VMEM, VMEM, VMEM],
        out_specs=[VMEM] * 2,
        out_shape=[jax.ShapeDtypeStruct((rows, pixels), jnp.float32)] * 2,
        scratch_shapes=[
            pltpu.VMEM((entries, pixels), kernel.dtype),
            partial, partial, factor, factor,
            pltpu.SemaphoreType.DMA((steps,)),
        ],
        compiler_params=ROOM,
        name="project",
    )(me, ends, place, kernel, *factors, slot, head)


def pack_kernel(cap, both, me_ref, mine_ref, other_ref, *outs):
    size = cap + HEAD
    lists = -(-both // LANES)
    lower = me_ref[2] == 0
    line = iota((HEAD, LANES), 0)
    heads, spilled = [], jnp.zeros((1, LANES), jnp.float32)
    for k, out in enumerate(outs):
        mine, other = mine_ref[k * size : (k + 1) * size, :], other_ref[k * size : (k + 1) * size, :]
        one, two = jnp.where(lower, mine, other), jnp.where(lower, other, mine)
        out[:cap, :] = one[:cap]
        if both > 2 * cap:
            out[cap : both - cap, :] = jnp.zeros((both - 2 * cap, LANES), jnp.float32)
        shared = max(2 * cap - both, 0)
        if shared:
            out[cap - shared : cap, :] = one[cap - shared : cap] + two[:shared]
        out[cap + max(both - 2 * cap, 0) : both, :] = two[shared:cap]
        head = one[cap:] + two[cap:]
        heads.append(head)
        spilled = spilled + head[lists : lists + 1] + jnp.maximum(head[lists + 1 : lists + 2] - both, 0.0)
    for out, head in zip(outs, heads):
        out[both:, :] = jnp.where(line == lists, spilled, head)


def pack(me, mine, other, cap, both):
    count = mine.shape[0] // (cap + HEAD)
    out = jax.ShapeDtypeStruct((both + HEAD, mine.shape[1]), jnp.float32)
    return pl.pallas_call(
        functools.partial(pack_kernel, cap, both),
        in_specs=[SMEM, VMEM, VMEM],
        out_specs=[VMEM] * count,
        out_shape=[out] * count,
        compiler_params=ROOM,
        name="pack",
    )(me, mine, other)


def split(x):
    high = x.astype(jnp.bfloat16)
    return high, (x - high.astype(jnp.float32)).astype(jnp.bfloat16)


def collect_kernel(count, sub_tiles, *refs):
    messages, outs, rows_s = refs[:count], refs[count : count + SUBS], refs[count + SUBS :]
    both, pixels = messages[0].shape[0] - HEAD, messages[0].shape[1]
    lists = -(-both // LANES)
    flag = jnp.zeros((HEAD, pixels), jnp.float32)
    ids = []
    for message, rows in zip(messages, rows_s):
        rows[...] = jnp.concatenate(split(message[:both, :]), axis=1)
        head = message[both:, :]
        flag = flag + head[lists : lists + 1]
        names = jnp.concatenate([head[i : i + 1] for i in range(lists)], axis=1)[:, :both]
        ids.append(names.astype(jnp.int32) - 1)
    chunk = min(256, sub_tiles)
    for sub, out_ref in enumerate(outs):
        for t in range(0, sub_tiles, chunk):
            sums = jnp.zeros((chunk, 2 * pixels), jnp.float32)
            for names, rows in zip(ids, rows_s):
                hit = ones_where(iota((chunk, both), 0) + (sub * sub_tiles + t) == names)
                sums = sums + dot(hit, rows[...])
            out_ref[t : t + chunk, :] = sums[:, :pixels] + sums[:, pixels:]
        out_ref[sub_tiles:, :] = flag


def collect(messages, sub_tiles):
    rows, pixels = messages[0].shape
    return pl.pallas_call(
        functools.partial(collect_kernel, len(messages), sub_tiles),
        in_specs=[VMEM] * len(messages),
        out_specs=[VMEM] * SUBS,
        out_shape=[jax.ShapeDtypeStruct((sub_tiles + HEAD, pixels), jnp.float32)] * SUBS,
        scratch_shapes=[pltpu.VMEM((rows - HEAD, 2 * pixels), jnp.bfloat16)] * len(messages),
        compiler_params=ROOM,
        name="collect",
    )(*messages)


def owner_kernel(parts, me_ref, owner_ref, row_ref):
    most = row_ref.shape[1]
    owners = owner_ref[...]
    rows = owners.shape[0]
    mine = owners == me_ref[1] * 2 + me_ref[2]
    marks = jnp.where(mine, 1.0, 0.0)
    rank = running_counts(marks.astype(jnp.bfloat16), rows).astype(jnp.int32) - 1
    index = iota((rows, LANES), 0) * LANES + iota((rows, LANES), 1)
    found = jnp.zeros((HEAD, most), jnp.float32)
    line = iota((HEAD, LANES), 0)
    high, low = bytes_of(index + 1)
    for r in range(rows):
        pieces = jnp.where(line == 0, high[r : r + 1], jnp.where(line == 1, low[r : r + 1], 0.0))
        pieces = jnp.where(mine[r : r + 1], pieces, 0.0)
        spots = ones_where(iota((most, LANES), 0) == rank[r : r + 1])
        found = found + nt_dot(pieces.astype(jnp.bfloat16), spots)
    tile = (found[0:1] * 256.0 + found[1:2]).astype(jnp.int32) - 1
    tile = jnp.where(tile < 0, rows * LANES, tile)
    bounds = jnp.zeros((1, most), jnp.float32)
    for p in range(1, SUBS * parts + 1):
        before = jnp.where(index < p * (rows * LANES // (SUBS * parts)), marks, 0.0)
        bounds = jnp.where(iota((1, most), 1) == p, jnp.sum(before, axis=(0, 1), keepdims=True), bounds)
    row_ref[...] = jnp.where(iota((HEAD, most), 0) == 0, tile, bounds.astype(jnp.int32))


def owned_rows(me, owners, most, parts):
    return pl.pallas_call(
        functools.partial(owner_kernel, parts),
        in_specs=[SMEM, VMEM],
        out_specs=VMEM,
        out_shape=jax.ShapeDtypeStruct((HEAD, most), jnp.int32),
        compiler_params=ROOM,
        name="owned_rows",
    )(me, owners)


def fill_rows(row_ref, moves, start, end, shift):
    unroll = 8

    def one(r):
        at = pl.ds(row_ref[r] - shift, 1)
        for table, rows in moves:
            rows[pl.ds(r, 1), :] = table[at, :]

    def group(i, carry):
        for u in range(unroll):
            one(start + i * unroll + u)
        return carry

    def rest(r, carry):
        one(r)
        return carry

    groups = (end - start) // unroll
    lax.fori_loop(0, groups, group, 0)
    lax.fori_loop(start + groups * unroll, end, rest, 0)


def fill_part(m, sub, me_ref, row_ref, moves):
    most = moves[0][1].shape[0]
    tiles = moves[0][0].shape[0] - HEAD
    at = (me_ref[1] ^ m) * SUBS + sub
    fill_rows(row_ref, moves, row_ref[most + at], row_ref[most + at + 1], at * tiles)


def early_kernel(me_ref, row_ref, *refs):
    pieces, (own_rows, other_rows, flag_ref) = refs[:-3], refs[-3:]
    own, other = pieces[:SUBS], pieces[SUBS:]
    tiles = own[0].shape[0] - HEAD
    flag_ref[0] = jnp.max(own[0][tiles:, :]).astype(jnp.int32)
    own_rows[...] = jnp.zeros_like(own_rows)
    other_rows[...] = jnp.zeros_like(other_rows)
    for sub in range(SUBS):
        fill_part(0, sub, me_ref, row_ref, ((own[sub], own_rows), (other[sub], other_rows)))


def early(me, rows, own, other, most):
    out = jax.ShapeDtypeStruct((most, own[0].shape[1]), jnp.float32)
    return pl.pallas_call(
        early_kernel,
        in_specs=[SMEM, SMEM] + [VMEM] * (2 * SUBS),
        out_specs=[VMEM, VMEM, SMEM],
        out_shape=[out, out, jax.ShapeDtypeStruct((1,), jnp.int32)],
        compiler_params=ROOM,
        name="early",
    )(me, rows, *own, *other)


def middle_kernel(me_ref, row_ref, before_ref, *refs):
    pieces, rows_ref = refs[:-1], refs[-1]
    rows_ref[...] = before_ref[...]
    for i, piece in enumerate(pieces):
        fill_part(1 + i // SUBS, i % SUBS, me_ref, row_ref, ((piece, rows_ref),))


def middle(me, rows, before, pieces):
    return pl.pallas_call(
        middle_kernel,
        in_specs=[SMEM, SMEM, VMEM] + [VMEM] * len(pieces),
        out_specs=VMEM,
        out_shape=jax.ShapeDtypeStruct(before.shape, jnp.float32),
        compiler_params=ROOM,
        name="middle",
    )(me, rows, before, *pieces)


def late_kernel(me_ref, row_ref, own_rows, before_ref, *refs):
    pieces, (owned_ref, map_ref, other_rows) = refs[:-3], refs[-3:]
    tiles, pixels = pieces[0].shape[0] - HEAD, pieces[0].shape[1]
    half = len(pieces) // 2
    lower = me_ref[2] == 0

    def put(ref, at, own, other):
        ref[at, :pixels] = jnp.where(lower, own, other)
        ref[at, pixels:] = jnp.where(lower, other, own)

    other_rows[...] = before_ref[...]
    for i in range(half):
        own, other = pieces[i], pieces[half + i]
        m, sub = i // SUBS, i % SUBS
        at = pl.multiple_of(((me_ref[1] ^ m) * SUBS + sub) * tiles, tiles)
        put(map_ref, pl.ds(at, tiles), own[:tiles, :], other[:tiles, :])
        if m:
            fill_part(m, sub, me_ref, row_ref, ((other, other_rows),))
    put(owned_ref, slice(None), own_rows[...], other_rows[...])


def late(me, rows, own_rows, before, own, other, block):
    most, pixels = own_rows.shape
    return pl.pallas_call(
        late_kernel,
        in_specs=[SMEM, SMEM] + [VMEM] * (2 + len(own) + len(other)),
        out_specs=[VMEM, VMEM],
        out_shape=[
            jax.ShapeDtypeStruct((most, 2 * pixels), jnp.float32),
            jax.ShapeDtypeStruct((block, 2 * pixels), jnp.float32),
        ],
        scratch_shapes=[pltpu.VMEM((most, pixels), jnp.float32)],
        compiler_params=ROOM,
        name="late",
    )(me, rows, own_rows, before, *own, *other)


def shards(kernel, pressure, velocity, entry_slot, slot_tile, tile_owner):
    vols = lax.axis_size("vol")
    pixs = lax.axis_size("pix")
    vol = lax.axis_index("vol")
    pix = lax.axis_index("pix")
    entries, _ = kernel.shape
    slots = slot_tile.shape[1]
    block = tile_owner.shape[0] // vols
    parts = pixs // 2
    part_tiles = block // parts
    half = vols // 2
    most_owned = 2 * block // pixs
    most_rows = min(2 * slots // vols, part_tiles)
    me = jnp.stack([vol, pix >> 1, pix & 1]).astype(jnp.int32)
    tiles = slot_tile.reshape(slots // LANES, LANES)
    slot = entry_slot.reshape(entries // LANES, LANES)
    factors = [x.reshape(entries // LANES, LANES) for x in (pressure, velocity)]
    owners = lax.dynamic_slice_in_dim(
        tile_owner.reshape(vols, block // LANES, LANES), vol, 1
    )[0]
    rows = owned_rows(me, owners, most_owned, parts)[:2].reshape(-1)

    def send(x, vol_step=0, part_step=0, core_step=0):
        step = (vol_step * parts + part_step) * 2 + core_step
        return lax.ppermute(x, ("vol", "pix"), [(d, d ^ step) for d in range(vols * pixs)])

    def exchange(cap, both):
        count = half * parts
        place, ends, head = plan(me, tiles, slot, vols, parts, block, cap, both)
        own, given = project(
            me, kernel, factors, slot, ends.reshape(-1), place.reshape(-1), head, cap
        )
        messages = pack(me, own, send(given, core_step=1), cap, both)

        def gather(messages):
            messages = list(messages)
            for k in reversed(range(1, count)):
                messages[k] = send(messages[k], k // parts, k % parts)
            return collect(messages, part_tiles // SUBS)

        far = gather(messages[count:])
        crossed = [send(x, vol_step=half) for x in far]
        near = gather(messages[:count])
        mine = [x + y for x, y in zip(near, crossed)]
        other = [send(x, core_step=1) for x in mine]
        own_rows, other_rows, flag = early(me, rows, mine, other, most_owned)
        across = [send(x, part_step=m) for m in range(1, parts) for x in mine]
        beyond = [send(x, core_step=1) for x in across]
        own_rows = middle(me, rows, own_rows, across)
        full = late(me, rows, own_rows, other_rows, mine + across, other + beyond, block)
        return flag[0] > 0, *full

    def rows_of(share):
        return most_rows * share // 32 // 8 * 8

    result = exchange(rows_of(13), rows_of(24))

    def redo(state):
        unused, *full = exchange(most_rows, 2 * most_rows)
        return jnp.zeros((), bool), *full

    _, owned, shell = lax.while_loop(lambda state: state[0], redo, result)
    return owned, shell


def solution(mesh):
    in_specs = (
        P(("vol", "pix"), None),
        P(("vol", "pix")),
        P(("vol", "pix")),
        P(("vol", "pix"), None),
        P(("vol", "pix"), None),
        P(),
    )
    out_specs = (P(("vol", "pix"), None), P("vol", None))
    return jax.shard_map(shards, mesh=mesh, in_specs=in_specs, out_specs=out_specs, check_vma=False)
```
